512 devices in a mesh: tok: 8 (over x, core), voc: 64 (over z, y).
Axes of the slice: x: 4, y: 8, z: 8, core: 2. Of those that a mesh axis runs over, the one named last changes fastest.
Arguments:
- hidden: bfloat16 [1024, 4608], P(('tok', 'voc')), may hold values from -6 to 6
- norm_gain: float32 [4608], replicated, may hold values from 0.25 to 1.75
- head_weight: bfloat16 [262144, 4608], P(('tok', 'voc')), may hold values from -0.26367188 to 0.26367188
- targets: int32 [1024], replicated, may hold values from 0 to 262143
- lengths: int32 [32], replicated, may hold values from 1 to 32
Outputs:
- token_loss: float32 [1024], P(('tok', 'voc'))
- mean_loss: float32 [], replicated
The draws below stay inside these ranges and needn't reach their ends.
All inputs are finite; a program needn't handle non-finite values.
Results may differ from the reference program's by a relative error of at most 0.00051.
Values may be sent and summed in bfloat16 or wider, within the bound.
No kernel may reach another device: no remote copies, remote signals or barrier semaphores. Data moves between devices by JAX's collectives and lax.ppermute only.
A program may use at most 64 MiB of HBM per device.

```python
import jax
import jax.numpy as jnp
from jax import lax

D = 4608
VOC_DEV = 512
WINDOW = 32
VOCAB = 262144
TOKENS = 1024
SEQS = 32


def plant(values, stream_key, least, top_value):
    shape = values.shape
    place = [jax.random.randint(jax.random.fold_in(stream_key, axis), (), 0, shape[axis]) for axis in range(len(shape))]
    values = values.at[tuple(place)].set(least)
    longest = shape.index(max(shape))
    place[longest] = (place[longest] + 1) % shape[longest]
    return values.at[tuple(place)].set(top_value)


def block_scale(rng, shape, shards, low, high):
    level = 1.0
    for dim, parts in shards:
        draws = jax.random.uniform(jax.random.fold_in(jax.random.fold_in(rng, 6), dim), (parts,), jnp.float32, low / len(shards), high / len(shards))
        level = level * jnp.repeat(jnp.exp(draws), shape[dim] // parts).reshape((-1,) + (1,) * (len(shape) - 1 - dim))
    return level


def scatter_about(own_key, dims, width, bound, split=(), held_as=jnp.bfloat16):
    values = jax.random.normal(own_key, dims, jnp.float32) * width
    if len(split) > 0:
        values = block_scale(own_key, dims, split, -0.22, 0.18) * values
    return jnp.clip(values, min=-bound, max=bound).astype(held_as)


def setup_inputs(seed: int = 0) -> dict:
    streams_of = jax.random.split(jax.random.key(seed), 6)
    hidden = scatter_about(streams_of[0], (TOKENS, D), 1.0, 6.0, ((0, 512),))
    norm_gain = jnp.clip(1.0 + 0.15 * jax.random.normal(streams_of[1], (D,), jnp.float32), 0.25, 1.75)
    head_weight = scatter_about(streams_of[2], (VOCAB, D), (3.0 * D ** -0.5), 0.26367188, ((0, 512),))
    targets = plant(jax.random.randint(streams_of[3], (TOKENS,), 0, VOCAB), jax.random.fold_in(streams_of[3], 1), 0, VOCAB - 1).astype(jnp.int32)
    lengths = plant(jax.random.randint(streams_of[4], (SEQS,), 1, WINDOW + 1), jax.random.fold_in(streams_of[4], 1), 1, WINDOW).astype(jnp.int32)
    return {"hidden": hidden, "norm_gain": norm_gain, "head_weight": head_weight, "targets": targets, "lengths": lengths}


def reference(hidden, norm_gain, head_weight, targets, lengths):
    values = hidden.astype(jnp.float32)
    meansq = lax.optimization_barrier(jnp.mean(values * values, axis=1, keepdims=True))
    normed = (values * lax.rsqrt(meansq + 1e-06) * norm_gain[None, :]).astype(jnp.bfloat16)
    blocks = head_weight.reshape(VOCAB // VOC_DEV, VOC_DEV, D)
    count = VOCAB // VOC_DEV

    def step(carry, item):
        expsum, picked = carry
        block, number = item
        logits = lax.dot_general(normed, block, (((1,), (1,)), ((), ())), preferred_element_type=jnp.float32)
        capped = 30.0 * jnp.tanh(logits / 30.0)
        expsum = expsum + lax.optimization_barrier(jnp.sum(jnp.exp(capped), axis=1))
        local = targets - number * VOC_DEV
        column = jnp.arange(VOC_DEV, dtype=jnp.int32)
        match = column[None, :] == local[:, None]
        picked = picked + lax.optimization_barrier(jnp.sum(jnp.where(match, capped, jnp.zeros_like(capped)), axis=1))
        return ((expsum, picked), None)
    start = (jnp.zeros((TOKENS,), jnp.float32), jnp.zeros((TOKENS,), jnp.float32))
    (expsum, picked), _ = lax.scan(step, start, (blocks, jnp.arange(count, dtype=jnp.int32)))
    position = jnp.arange(WINDOW, dtype=jnp.int32)
    live = (position[None, :] < lengths[:, None]).astype(jnp.float32).reshape(TOKENS)
    token_loss = live * (jnp.log(expsum) - picked)
    mean_loss = jnp.sum(token_loss) / jnp.sum(lengths.astype(jnp.float32))
    return (token_loss, mean_loss)
```

```python
import jax
import jax.numpy as jnp
from jax import lax
from jax.experimental import pallas as pl
from jax.experimental.pallas import tpu as pltpu
from jax.sharding import Mesh
from jax.sharding import PartitionSpec as P

WINDOW = 32
TOK_VOC = ("x", "c", "z", "y")
PLANE = ("z", "y")
K_TILE = 1536
ROWS = 64


def head_kernel(place, targets, *refs):
    n = (len(refs) - 4)
    xs, (w0, w1, out, acc) = refs[:n], refs[n:]
    step = pl.program_id(0)
    rows = jnp.concatenate([x[...] for x in xs], axis=0)
    for shard, w in enumerate((w0, w1)):
        part = lax.dot_general(w[...], rows, (((1,), (1,)), ((), ())), preferred_element_type=jnp.float32)

        @pl.when(step == 0)
        def _():
            acc[shard] = part

        @pl.when(step > 0)
        def _():
            acc[shard] += part

    @pl.when(step == pl.num_programs(0) - 1)
    def _():
        core = place[0]
        wanted = [targets[pl.ds(place[3 + k] * 2 + core, 1), :] for k in range(n)]
        wanted = jnp.concatenate(wanted, axis=1)
        tokens = wanted.shape[1]
        vocab = w0.shape[0]
        expsum = jnp.zeros((8, tokens), jnp.float32)
        picked = jnp.zeros((8, tokens), jnp.float32)
        for shard in range(2):
            local = wanted - place[1 + shard]
            for r in range(0, vocab, ROWS):
                capped = 30.0 * jnp.tanh(acc[shard, r:r + ROWS, :] / 30.0)
                column = lax.broadcasted_iota(jnp.int32, (ROWS, tokens), 0) + r
                hit = jnp.where(column == local, capped, 0.0)
                expsum += jnp.sum(jnp.exp(capped).reshape(ROWS // 8, 8, tokens), axis=0)
                picked += jnp.sum(hit.reshape(ROWS // 8, 8, tokens), axis=0)
        expsum = jnp.sum(expsum, axis=0, keepdims=True)
        picked = jnp.sum(picked, axis=0, keepdims=True)
        for k in range(n):
            out[pl.ds(place[3 + k], 1), :] = expsum[:, k * 128:(k + 1) * 128]
            out[pl.ds(place[3 + k] + n, 1), :] = picked[:, k * 128:(k + 1) * 128]


def head(place, targets, blocks, w0, w1):
    n = len(blocks)
    depth = w0.shape[1]
    vocab = w0.shape[0]
    k_tile = K_TILE
    block = blocks[0].shape[0]
    return pl.pallas_call(
        head_kernel,
        grid=(depth // k_tile,),
        in_specs=[pl.BlockSpec(memory_space=pltpu.SMEM), pl.BlockSpec(targets.shape, lambda k: (0, 0))]
        + [pl.BlockSpec((block, k_tile), lambda k: (0, k))] * n
        + [pl.BlockSpec((vocab, k_tile), lambda k: (0, k))] * 2,
        out_specs=pl.BlockSpec((2 * n, 128), lambda k: (0, 0)),
        out_shape=jax.ShapeDtypeStruct((2 * n, 128), jnp.float32),
        scratch_shapes=[pltpu.VMEM((2, vocab, n * block), jnp.float32)],
        compiler_params=pltpu.CompilerParams(dimension_semantics=("arbitrary",), vmem_limit_bytes=40 * 2**20),
        cost_estimate=pl.CostEstimate(flops=4 * vocab * n * block * depth, bytes_accessed=14 * 2**20, transcendentals=0),
        name="head",
    )(place, targets, *blocks, w0, w1)


def spread(value, axes, count):
    return lax.all_to_all(jnp.broadcast_to(value[None], (count, *value.shape)), axes, 0, 0)


def body(hidden, norm_gain, head_weight, targets, lengths):
    own_rows = hidden.shape[0]
    vocab_rows = head_weight.shape[0]
    nx, nc = lax.axis_size("x"), lax.axis_size("c")
    plane = lax.axis_size(PLANE)
    x, c = lax.axis_index("x"), lax.axis_index("c")
    seat = lax.axis_index(PLANE)
    block = plane * own_rows

    values = hidden.astype(jnp.float32)
    meansq = jnp.mean(values * values, axis=1, keepdims=True)
    normed = (values * lax.rsqrt(meansq + 1e-06) * norm_gain[None, :]).astype(jnp.bfloat16)

    other_weight = lax.ppermute(head_weight, "c", [(0, 1), (1, 0)])
    mine = spread(normed, PLANE, plane).reshape(block, -1)
    turns = (0, 1, nx - 1, 2)
    blocks = [mine if k == 0 else lax.ppermute(mine, "x", [(i, (i + k) % nx) for i in range(nx)]) for k in turns]
    sources = [lax.rem(x + nx - k, nx) for k in turns]
    first = ((x * nc + c) * plane + seat) * vocab_rows
    second = ((x * nc + 1 - c) * plane + seat) * vocab_rows
    place = jnp.stack([c, first, second, *sources]).astype(jnp.int32)
    stats = head(place, targets.reshape(nx * nc, block), blocks, head_weight, other_weight)

    stats = jnp.sum(spread(stats, PLANE, plane), axis=0)
    stats = spread(stats, ("x", "c"), nx * nc).reshape(nx, nc, 2, nx, block)
    totals = jnp.sum(stats, axis=0)
    totals = totals.transpose(1, 2, 0, 3)
    position = jnp.arange(WINDOW, dtype=jnp.int32)
    live = (position[None, :] < lengths[:, None]).astype(jnp.float32).reshape(nx, nc, block)
    count = jnp.sum(lengths.astype(jnp.float32))
    loss = live * (jnp.log(totals[0]) - totals[1])
    mean_loss = jnp.sum(loss) / count
    token_loss = lax.dynamic_slice(loss, (x, c, seat * own_rows), (1, 1, own_rows)).reshape(own_rows)
    return (token_loss, mean_loss)


def solution(mesh):
    split = Mesh(mesh.devices.reshape(4, 2, 8, 8), TOK_VOC)
    in_specs = (P(TOK_VOC, None), P(), P(TOK_VOC, None), P(), P())
    out_specs = (P(TOK_VOC), P())
    return jax.shard_map(body, mesh=split, in_specs=in_specs, out_specs=out_specs, check_vma=False)
```

```python
import jax
import jax.numpy as jnp
from jax import lax
from jax.experimental import pallas as pl
from jax.experimental.pallas import tpu as pltpu
from jax.sharding import Mesh
from jax.sharding import PartitionSpec as P

WINDOW = 32
TOK_VOC = ("x", "c", "z", "y")
PLANE = ("z", "y")
WIDE = 3328
ROWS = 256
STRIP = 64


def dot_t(a, b):
    return lax.dot_general(a, b, (((1,), (1,)), ((), ())), preferred_element_type=jnp.float32)


def first_kernel(*refs):
    xs, (w0, w1, out) = refs[:-3], refs[-3:]
    half = pl.num_programs(0) // 2
    rows = jnp.concatenate([x[...] for x in xs], axis=0)

    @pl.when(pl.program_id(0) < half)
    def _():
        out[...] = dot_t(w0[...], rows)

    @pl.when(pl.program_id(0) >= half)
    def _():
        out[...] = dot_t(w1[...], rows)


def second_kernel(place, targets, near, far0, far1, mixed, w0, w1, out, sorted_rows, logits, sums):
    step = pl.program_id(0)
    half = pl.num_programs(0) // 2
    wide = far0.shape[1]
    tokens = mixed.shape[0]
    groups = tokens // 128

    @pl.when(step == 0)
    def _():
        row = lax.broadcasted_iota(jnp.int32, (tokens, tokens), 0)
        col = lax.broadcasted_iota(jnp.int32, (tokens, tokens), 1)
        inner = row & 127
        pick = (inner >> 1) * (2 * groups) + (row >> 7) * 2 + (inner & 1)
        chosen = jnp.where(col == pick, 1.0, 0.0).astype(jnp.bfloat16)
        sorted_rows[...] = jnp.dot(chosen, mixed[...], preferred_element_type=jnp.float32).astype(jnp.bfloat16)
        sums[...] = jnp.zeros_like(sums)

    far = jnp.concatenate([far0[...], far1[...]], axis=0)
    known = near.shape[1]

    def multiply(w):
        part = dot_t(w[:, wide:], sorted_rows[...])
        logits[:, :known] = part[:, :known] + near[...]
        logits[:, known:] = part[:, known:] + dot_t(w[:, :wide], far)

    @pl.when(step < half)
    def _():
        multiply(w0)

    @pl.when(step >= half)
    def _():
        multiply(w1)

    core = place[0]
    wanted = [targets[pl.ds(place[3 + k] * 2 + core, 1), :] for k in range(groups)]
    start = jnp.where(step < half, place[1], place[2]) + lax.rem(step, half) * logits.shape[0]
    local = jnp.concatenate(wanted, axis=1) - start
    expsum = sums[0]
    picked = sums[1]
    for r in range(0, logits.shape[0], STRIP):
        capped = 30.0 * jnp.tanh(logits[r:r + STRIP, :] / 30.0)
        column = lax.broadcasted_iota(jnp.int32, (STRIP, tokens), 0) + r
        hit = jnp.where(column == local, capped, 0.0)
        expsum += jnp.sum(jnp.exp(capped).reshape(STRIP // 8, 8, tokens), axis=0)
        picked += jnp.sum(hit.reshape(STRIP // 8, 8, tokens), axis=0)
    sums[0] = expsum
    sums[1] = picked

    @pl.when(step == pl.num_programs(0) - 1)
    def _():
        for stat in range(2):
            total = jnp.sum(sums[stat], axis=0, keepdims=True)
            for k in range(groups):
                out[pl.ds(place[3 + k] + stat * groups, 1), :] = total[:, k * 128:(k + 1) * 128]


def whole(shape):
    return pl.BlockSpec(shape, lambda i: (0,) * len(shape))


def weight_specs(vocab, width):
    half = vocab // ROWS
    return [
        pl.BlockSpec((ROWS, width), lambda i: (jnp.minimum(i, half - 1), 0)),
        pl.BlockSpec((ROWS, width), lambda i: (jnp.maximum(i - half, 0), 0)),
    ]


def first_product(xs, w0, w1):
    vocab = w0.shape[0]
    wide = xs[0].shape[1]
    tokens = sum(x.shape[0] for x in xs)
    return pl.pallas_call(
        first_kernel,
        grid=(2 * vocab // ROWS,),
        in_specs=[whole(x.shape) for x in xs] + weight_specs(vocab, wide),
        out_specs=pl.BlockSpec((ROWS, tokens), lambda i: (i, 0)),
        out_shape=jax.ShapeDtypeStruct((2 * vocab, tokens), jnp.float32),
        compiler_params=pltpu.CompilerParams(dimension_semantics=("arbitrary",), vmem_limit_bytes=52 * 2**20),
        cost_estimate=pl.CostEstimate(flops=4 * vocab * tokens * wide, bytes_accessed=12 * 2**20, transcendentals=0),
        name="first_product",
    )(*xs, w0, w1)


def second_product(place, targets, near, far0, far1, mixed, w0, w1):
    vocab, depth = w0.shape
    tokens, narrow = mixed.shape
    groups = tokens // 128
    return pl.pallas_call(
        second_kernel,
        grid=(2 * vocab // ROWS,),
        in_specs=[pl.BlockSpec(memory_space=pltpu.SMEM), whole(targets.shape)]
        + [pl.BlockSpec((ROWS, near.shape[1]), lambda i: (i, 0)), whole(far0.shape), whole(far1.shape), whole(mixed.shape)]
        + weight_specs(vocab, depth),
        out_specs=whole((2 * groups, 128)),
        out_shape=jax.ShapeDtypeStruct((2 * groups, 128), jnp.float32),
        scratch_shapes=[
            pltpu.VMEM((tokens, narrow), jnp.bfloat16),
            pltpu.VMEM((ROWS, tokens), jnp.float32),
            pltpu.VMEM((2, 8, tokens), jnp.float32),
        ],
        compiler_params=pltpu.CompilerParams(dimension_semantics=("arbitrary",), vmem_limit_bytes=52 * 2**20),
        cost_estimate=pl.CostEstimate(flops=2 * vocab * tokens * depth, bytes_accessed=14 * 2**20, transcendentals=0),
        name="second_product",
    )(place, targets, near, far0, far1, mixed, w0, w1)


def spread(value, axes):
    count = lax.axis_size(axes)
    return lax.all_to_all(jnp.broadcast_to(value[None], (count, *value.shape)), axes, 0, 0)


def body(hidden, norm_gain, head_weight, targets, lengths):
    own_rows = hidden.shape[0]
    vocab_rows = head_weight.shape[0]
    nx, nc = lax.axis_size("x"), lax.axis_size("c")
    plane = lax.axis_size(PLANE)
    x, c = lax.axis_index("x"), lax.axis_index("c")
    seat = lax.axis_index(PLANE)
    block = plane * own_rows

    def turn(value, k):
        return lax.ppermute(value, "x", [(i, (i + k) % nx) for i in range(nx)])

    values = hidden.astype(jnp.float32)
    meansq = jnp.mean(values * values, axis=1, keepdims=True)
    normed = (values * lax.rsqrt(meansq + 1e-06) * norm_gain[None, :]).astype(jnp.bfloat16)
    mine = spread(normed[:, :WIDE], PLANE).reshape(block, WIDE)
    other_weight = lax.ppermute(head_weight, "c", [(0, 1), (1, 0)])
    narrow = normed[:, WIDE:]
    column = jnp.concatenate([narrow, turn(narrow, 1), turn(narrow, nx - 1), turn(narrow, 2)], axis=0)
    mixed = spread(column, PLANE).reshape(nx * block, -1)
    low, high = mine[:block // 2], mine[block // 2:]
    up_low, down_high = turn(low, 1), turn(high, nx - 1)
    up_high, down_low = turn(high, 1), turn(low, nx - 1)
    far_low, far_high = turn(up_low, 1), turn(down_high, nx - 1)
    near = first_product((mine, up_low, up_high, down_low, down_high), head_weight, other_weight)
    sources = [lax.rem(x + nx - k, nx) for k in (0, 1, nx - 1, 2)]
    first = ((x * nc + c) * plane + seat) * vocab_rows
    second = ((x * nc + 1 - c) * plane + seat) * vocab_rows
    place = jnp.stack([c, first, second, *sources]).astype(jnp.int32)
    stats = second_product(
        place, targets.reshape(nx * nc, block), near, far_low, far_high, mixed, head_weight, other_weight
    )
    stats = jnp.sum(spread(stats, ("x", "z")), axis=0)
    stats = spread(stats, ("c", "y"))
    totals = jnp.sum(stats.reshape(nc, -1, 2, nx, block), axis=1).transpose(1, 2, 0, 3)
    position = jnp.arange(WINDOW, dtype=jnp.int32)
    live = (position[None, :] < lengths[:, None]).astype(jnp.float32).reshape(nx, nc, block)
    count = jnp.sum(lengths.astype(jnp.float32))
    loss = live * (jnp.log(totals[0]) - totals[1])
    mean_loss = jnp.sum(loss) / count
    token_loss = lax.dynamic_slice(loss, (x, c, seat * own_rows), (1, 1, own_rows)).reshape(own_rows)
    return (token_loss, mean_loss)


def solution(mesh):
    split = Mesh(mesh.devices.reshape(4, 2, 8, 8), TOK_VOC)
    in_specs = (P(TOK_VOC, None), P(), P(TOK_VOC, None), P(), P())
    out_specs = (P(TOK_VOC), P())
    return jax.shard_map(body, mesh=split, in_specs=in_specs, out_specs=out_specs, check_vma=False)
```

```python
import jax
import jax.numpy as jnp
from jax import lax
from jax.experimental import pallas as pl
from jax.experimental.pallas import tpu as pltpu
from jax.sharding import Mesh
from jax.sharding import PartitionSpec as P

WINDOW = 32
TOK_VOC = ("x", "c", "z", "y")
PLANE = ("z", "y")
WIDE = 3584
TILE = 512
STRIP = 64
VMEM_LIMIT = 46 * 2**20


def params(serial=False):
    order = {"dimension_semantics": ("arbitrary",)} if serial else {}
    return pltpu.CompilerParams(vmem_limit_bytes=VMEM_LIMIT, **order)


def whole(shape):
    return pl.BlockSpec(shape, lambda *_: (0,) * len(shape))


def scalars():
    return pl.BlockSpec(memory_space=pltpu.SMEM)


def dot_t(a, b):
    return lax.dot_general(a, b, (((1,), (1,)), ((), ())), preferred_element_type=jnp.float32)


def norm_kernel(hidden, gain, wide, narrow):
    values = hidden[...].astype(jnp.float32)
    meansq = jnp.mean(values * values, axis=1, keepdims=True)
    normed = (values * lax.rsqrt(meansq + 1e-06) * gain[...]).astype(jnp.bfloat16)
    width = wide.shape[2]
    narrow[...] = normed[:, width:]
    for i in range(wide.shape[0]):
        wide[i] = normed[:, :width]


def norm(hidden, gain, copies, width):
    rows, depth = hidden.shape
    shapes = [(copies, rows, width), (rows, depth - width)]
    return pl.pallas_call(
        norm_kernel,
        in_specs=[whole(hidden.shape), whole((1, depth))],
        out_specs=[whole(s) for s in shapes],
        out_shape=[jax.ShapeDtypeStruct(s, jnp.bfloat16) for s in shapes],
        compiler_params=params(),
        name="norm",
    )(hidden, gain.reshape(1, depth))


def first_kernel(wide_steps, *refs):
    xs, (mixed, w0, w1, out) = refs[:-4], refs[-4:]
    step = pl.program_id(0)
    weight = jnp.concatenate([w0[...], w1[...]], axis=0)
    early = sum(x.shape[0] for x in xs)

    @pl.when(step < wide_steps)
    def _():
        part = dot_t(weight, jnp.concatenate([x[...] for x in xs], axis=0))

        @pl.when(step == 0)
        def _():
            out[:, :early] = part

        @pl.when(step > 0)
        def _():
            out[:, :early] += part

    @pl.when(step >= wide_steps)
    def _():
        tokens = mixed.shape[0]
        groups = tokens // 128
        row = lax.broadcasted_iota(jnp.int32, (tokens, tokens), 0)
        col = lax.broadcasted_iota(jnp.int32, (tokens, tokens), 1)
        inner = row & 127
        pick = (inner >> 1) * (2 * groups) + (row >> 7) * 2 + (inner & 1)
        chosen = jnp.where(col == pick, 1.0, 0.0).astype(jnp.bfloat16)
        rows = jnp.dot(chosen, mixed[...], preferred_element_type=jnp.float32).astype(jnp.bfloat16)
        part = dot_t(weight, rows)
        out[:, :early] += part[:, :early]

        @pl.when(step == wide_steps)
        def _():
            out[:, early:] = part[:, early:]

        @pl.when(step > wide_steps)
        def _():
            out[:, early:] += part[:, early:]


def first_product(xs, mixed, w0, w1):
    vocab, depth = w0.shape
    wide_steps = xs[0].shape[1] // TILE
    steps = depth // TILE
    tokens = mixed.shape[0]
    return pl.pallas_call(
        lambda *refs: first_kernel(wide_steps, *refs),
        grid=(steps,),
        in_specs=[pl.BlockSpec((x.shape[0], TILE), lambda k: (0, jnp.minimum(k, wide_steps - 1))) for x in xs]
        + [pl.BlockSpec((tokens, TILE), lambda k: (0, jnp.maximum(k - wide_steps, 0)))]
        + [pl.BlockSpec((vocab, TILE), lambda k: (0, k))] * 2,
        out_specs=whole((2 * vocab, tokens)),
        out_shape=jax.ShapeDtypeStruct((2 * vocab, tokens), jnp.float32),
        compiler_params=params(serial=True),
        cost_estimate=pl.CostEstimate(flops=2 * vocab * tokens * depth, bytes_accessed=14 * 2**20, transcendentals=0),
        name="first_product",
    )(*xs, mixed, w0, w1)


def second_kernel(place, targets, near, *refs):
    xs, (w0, w1, out, late, stat) = refs[:-5], refs[-5:]
    step = pl.program_id(0)
    vocab = w0.shape[0]
    early = near.shape[1] - late.shape[1]
    tokens = near.shape[1]
    groups = tokens // 128
    weight = jnp.concatenate([w0[...], w1[...]], axis=0)
    part = dot_t(weight, jnp.concatenate([x[...] for x in xs], axis=0))

    @pl.when(step == 0)
    def _():
        late[...] = near[:, early:] + part

    @pl.when(step > 0)
    def _():
        late[...] += part

    @pl.when(step == pl.num_programs(0) - 1)
    def _():
        wanted = jnp.concatenate([targets[pl.ds(place[3 + k] * 2 + place[0], 1), :] for k in range(groups)], axis=1)
        expsum = jnp.zeros((8, tokens), jnp.float32)
        picked = jnp.zeros((8, tokens), jnp.float32)
        for r in range(0, 2 * vocab, STRIP):
            logits = jnp.concatenate([near[r:r + STRIP, :early], late[r:r + STRIP, :]], axis=1)
            capped = 30.0 * jnp.tanh(logits / 30.0)
            local = wanted - (place[1 + r // vocab] + r % vocab)
            column = lax.broadcasted_iota(jnp.int32, (STRIP, tokens), 0)
            hit = jnp.where(column == local, capped, 0.0)
            expsum += jnp.sum(jnp.exp(capped).reshape(STRIP // 8, 8, tokens), axis=0)
            picked += jnp.sum(hit.reshape(STRIP // 8, 8, tokens), axis=0)
        for i, total in enumerate((expsum, picked)):
            total = jnp.sum(total, axis=0, keepdims=True)
            for k in range(groups):
                stat[pl.ds(place[3 + k] + i * groups, 1), :] = total[:, k * 128:(k + 1) * 128]
        for i in range(out.shape[0]):
            out[i] = stat[...]


def second_product(place, targets, near, xs, w0, w1, copies):
    vocab, _ = w0.shape
    wide = xs[0].shape[1]
    tokens = near.shape[1]
    late = sum(x.shape[0] for x in xs)
    rows = 2 * tokens // 128
    return pl.pallas_call(
        second_kernel,
        grid=(wide // TILE,),
        in_specs=[scalars(), whole(targets.shape), whole(near.shape)]
        + [pl.BlockSpec((x.shape[0], TILE), lambda k: (0, k)) for x in xs]
        + [pl.BlockSpec((vocab, TILE), lambda k: (0, k))] * 2,
        out_specs=whole((copies, rows, 128)),
        out_shape=jax.ShapeDtypeStruct((copies, rows, 128), jnp.float32),
        scratch_shapes=[pltpu.VMEM((2 * vocab, late), jnp.float32), pltpu.VMEM((rows, 128), jnp.float32)],
        compiler_params=params(serial=True),
        cost_estimate=pl.CostEstimate(flops=4 * vocab * late * wide, bytes_accessed=10 * 2**20, transcendentals=0),
        name="second_product",
    )(place, targets, near, *xs, w0, w1)


def join_kernel(parts, out):
    total = jnp.sum(parts[...], axis=0)
    for i in range(out.shape[0]):
        out[i] = total


def join(parts, copies):
    shape = (copies, *parts.shape[1:])
    return pl.pallas_call(
        join_kernel,
        in_specs=[whole(parts.shape)],
        out_specs=whole(shape),
        out_shape=jax.ShapeDtypeStruct(shape, jnp.float32),
        compiler_params=params(),
        name="join",
    )(parts)


def loss_kernel(place, count, live, parts, token_loss, mean_loss, loss):
    groups = parts.shape[1] // 2
    for core in range(2):
        total = parts[core]
        for i in range(core + 2, parts.shape[0], 2):
            total = total + parts[i]
        rows = slice(core * groups, (core + 1) * groups)
        loss[rows, :] = live[rows, :] * (jnp.log(total[:groups]) - total[groups:])
    mean_loss[0] = jnp.sum(loss[...]) / count[0]
    own = loss[pl.ds(place[0], 1), :]
    lane = lax.broadcasted_iota(jnp.int32, own.shape, 1)
    for i in range(token_loss.shape[0]):
        token_loss[i] = jnp.sum(jnp.where(lane == place[1] + i, own, 0.0))


def final_loss(place, count, live, parts, own_rows):
    return pl.pallas_call(
        loss_kernel,
        in_specs=[scalars(), scalars(), whole(live.shape), whole(parts.shape)],
        out_specs=[scalars(), scalars()],
        out_shape=[jax.ShapeDtypeStruct((own_rows,), jnp.float32), jax.ShapeDtypeStruct((1,), jnp.float32)],
        scratch_shapes=[pltpu.VMEM(live.shape, jnp.float32)],
        compiler_params=params(),
        name="final_loss",
    )(place, count, live, parts)


def exchange(value, axes):
    return lax.all_to_all(value, axes, 0, 0)


def body(hidden, norm_gain, head_weight, targets, lengths):
    own_rows = hidden.shape[0]
    vocab_rows = head_weight.shape[0]
    nx, nc = lax.axis_size("x"), lax.axis_size("c")
    plane = lax.axis_size(PLANE)
    x, c = lax.axis_index("x"), lax.axis_index("c")
    seat = lax.axis_index(PLANE)
    block = plane * own_rows

    def turn(value, k):
        return lax.ppermute(value, "x", [(i, (i + k) % nx) for i in range(nx)])

    wide, narrow = norm(hidden, norm_gain, plane, WIDE)
    mine = exchange(wide, PLANE).reshape(block, WIDE)
    other_weight = lax.ppermute(head_weight, "c", [(0, 1), (1, 0)])
    column = jnp.concatenate([narrow, turn(narrow, 1), turn(narrow, nx - 1), turn(narrow, 2)], axis=0)
    mixed = exchange(jnp.broadcast_to(column[None], (plane, *column.shape)), PLANE).reshape(nx * block, -1)
    low, high = mine[:block // 2], mine[block // 2:]
    up_low, down_high = turn(low, 1), turn(high, nx - 1)
    up_high, down_low = turn(high, 1), turn(low, nx - 1)
    far_low, far_high = turn(up_low, 1), turn(down_high, nx - 1)
    near = first_product((low, high, up_low, up_high), mixed, head_weight, other_weight)
    sources = [lax.rem(x + nx - k, nx) for k in (0, 1, nx - 1, 2)]
    first = ((x * nc + c) * plane + seat) * vocab_rows
    second = ((x * nc + 1 - c) * plane + seat) * vocab_rows
    place = jnp.stack([c, first, second, *sources]).astype(jnp.int32)
    stats = second_product(
        place, targets.reshape(nx * nc, block), near, (down_low, down_high, far_low, far_high),
        head_weight, other_weight, plane,
    )
    stats = join(exchange(stats, PLANE), nx * nc)
    stats = exchange(stats, ("x", "c"))
    position = jnp.arange(WINDOW, dtype=jnp.int32)
    live = (position[None, :] < lengths[:, None]).astype(jnp.float32).reshape(nx, nc, block)
    live = live.transpose(1, 0, 2).reshape(nx * nc, block)
    count = jnp.sum(lengths.astype(jnp.float32)).reshape(1)
    seat_of = jnp.stack([c * nx + x, seat * own_rows]).astype(jnp.int32)
    token_loss, mean_loss = final_loss(seat_of, count, live, stats, own_rows)
    return (token_loss, mean_loss.reshape(()))


def solution(mesh):
    split = Mesh(mesh.devices.reshape(4, 2, 8, 8), TOK_VOC)
    in_specs = (P(TOK_VOC, None), P(), P(TOK_VOC, None), P(), P())
    out_specs = (P(TOK_VOC), P())
    return jax.shard_map(body, mesh=split, in_specs=in_specs, out_specs=out_specs, check_vma=False)
```

```python
import jax
import jax.numpy as jnp
from jax import lax
from jax.experimental import pallas as pl
from jax.experimental.pallas import tpu as pltpu
from jax.sharding import Mesh
from jax.sharding import PartitionSpec as P

WINDOW = 32
TOK_VOC = ("x", "c", "z", "y")
PLANE = ("z", "y")
WIDE = 3584
STRIP = 64
CHUNKS = 2
VMEM_LIMIT = 12 * 2**20
WIDE_VMEM = 20 * 2**20


def params(limit=8 * 2**20):
    return pltpu.CompilerParams(vmem_limit_bytes=limit)


def whole(shape):
    return pl.BlockSpec(shape, lambda *_: (0,) * len(shape))


def scalars():
    return pl.BlockSpec(memory_space=pltpu.SMEM)


def dot_t(a, b):
    return lax.dot_general(a, b, (((1,), (1,)), ((), ())), preferred_element_type=jnp.float32)


def norm_kernel(hidden, gain, wide, narrow):
    values = hidden[...].astype(jnp.float32)
    meansq = jnp.mean(values * values, axis=1, keepdims=True)
    normed = (values * lax.rsqrt(meansq + 1e-06) * gain[...].reshape(1, -1)).astype(jnp.bfloat16)
    width = wide.shape[2]
    narrow[...] = normed[:, width:]
    for i in range(wide.shape[0]):
        wide[i] = normed[:, :width]


def norm(hidden, gain, copies, width):
    rows, depth = hidden.shape
    shapes = [(copies, rows, width), (rows, depth - width)]
    return pl.pallas_call(
        norm_kernel,
        in_specs=[whole(hidden.shape), whole(gain.shape)],
        out_specs=[whole(s) for s in shapes],
        out_shape=[jax.ShapeDtypeStruct(s, jnp.bfloat16) for s in shapes],
        compiler_params=params(),
        name="norm",
    )(in_hbm(hidden), in_hbm(gain))


def wanted_of(place, targets, groups):
    rows = [targets[pl.ds(place[3 + k] * 2 + place[0], 1), :] for k in groups]
    return jnp.concatenate(rows, axis=1)


def token_sums(place, wanted, logits):
    vocab, tokens = logits.shape
    expsum = jnp.zeros((8, tokens), jnp.float32)
    picked = jnp.zeros((8, tokens), jnp.float32)
    column = lax.broadcasted_iota(jnp.int32, (STRIP, tokens), 0)
    for r in range(0, vocab, STRIP):
        shard, offset = divmod(r, vocab // 2)
        capped = 30.0 * jnp.tanh(logits[r:r + STRIP, :] / 30.0)
        hit = jnp.where(column == wanted - (place[1 + shard] + offset), capped, 0.0)
        expsum += jnp.sum(jnp.exp(capped).reshape(STRIP // 8, 8, tokens), axis=0)
        picked += jnp.sum(hit.reshape(STRIP // 8, 8, tokens), axis=0)
    return jnp.sum(expsum, axis=0, keepdims=True), jnp.sum(picked, axis=0, keepdims=True)


def fetch(shards, kept, sems, starts, width):
    vocab = shards[0].shape[0]
    copies = []
    for i, start in enumerate(starts):
        pair = []
        for j, shard in enumerate(shards):
            source = shard.at[:, start:start + width]
            target = kept.at[j * vocab:(j + 1) * vocab, start:start + width]
            pair.append(pltpu.make_async_copy(source, target, sems.at[2 * i + j]))
            pair[-1].start()
        copies.append(pair)
    return copies


def first_kernel(place, targets, x0, x1, x2, x3, mixed, w0, w1, late, stat, kept, rows, logits, narrow_w, sems):
    wide = x0.shape[1]
    tokens, _ = mixed.shape
    groups = tokens // 128
    early = logits.shape[1]
    half = tokens // 2
    vocab = w0.shape[0]
    copies = [
        pltpu.make_async_copy(w.at[:, wide:], narrow_w.at[j * vocab:(j + 1) * vocab, :], sems.at[2 * CHUNKS + j])
        for j, w in enumerate((w0, w1))
    ]
    for copy in copies:
        copy.start()
    width = wide // CHUNKS
    others = fetch((w0, w1), kept, sems, [i * width for i in range(CHUNKS)], width)
    row = lax.broadcasted_iota(jnp.int32, (half, half), 0)
    col = lax.broadcasted_iota(jnp.int32, (half, half), 1)
    inner = row & 63
    pick = (inner >> 1) * (2 * groups) + (row >> 6) * 2 + (inner & 1)
    chosen = jnp.where(col == pick, 1.0, 0.0).astype(jnp.bfloat16)
    for h in range(2):
        part = jnp.dot(chosen, mixed[h * half:(h + 1) * half, :], preferred_element_type=jnp.float32)
        for k in range(groups):
            rows[k * 128 + h * 64:k * 128 + h * 64 + 64, :] = part[k * 64:(k + 1) * 64].astype(jnp.bfloat16)
    for copy in copies:
        copy.wait()
    late[...] = dot_t(narrow_w[...], rows[early:, :])
    logits[...] = dot_t(narrow_w[...], rows[:early, :])
    for i in range(CHUNKS):
        for copy in others[i]:
            copy.wait()
        cols = slice(i * width, (i + 1) * width)
        x = jnp.concatenate([x0[:, cols], x1[:, cols], x2[:, cols], x3[:, cols]], axis=0)
        logits[...] += dot_t(kept[:, cols], x)
    sums = token_sums(place, wanted_of(place, targets, (0, 1)), logits)
    for i, total in enumerate(sums):
        for k in range(2):
            stat[2 * i + k:2 * i + k + 1, :] = total[:, k * 128:(k + 1) * 128]


def first_product(place, targets, xs, mixed, w0, w1):
    vocab, depth = 2 * w0.shape[0], w0.shape[1]
    tokens, narrow = mixed.shape
    early = sum(x.shape[0] for x in xs)
    inside = pl.BlockSpec(memory_space=pltpu.VMEM)
    outside = pl.BlockSpec(memory_space=pltpu.HBM)
    return pl.pallas_call(
        first_kernel,
        in_specs=[scalars()] + [inside] * 6 + [outside] * 2,
        out_specs=[inside] * 3,
        out_shape=[
            jax.ShapeDtypeStruct((vocab, tokens - early), jnp.float32),
            jax.ShapeDtypeStruct((8, 128), jnp.float32),
            jax.ShapeDtypeStruct((vocab, depth - narrow), w0.dtype),
        ],
        scratch_shapes=[
            pltpu.VMEM((tokens, narrow), jnp.bfloat16),
            pltpu.VMEM((vocab, early), jnp.float32),
            pltpu.VMEM((vocab, narrow), w0.dtype),
            pltpu.SemaphoreType.DMA((2 * CHUNKS + 2,)),
        ],
        compiler_params=params(WIDE_VMEM),
        cost_estimate=pl.CostEstimate(flops=vocab * tokens * depth, bytes_accessed=14 * 2**20, transcendentals=0),
        name="first_product",
    )(place, targets, *xs, mixed, w0, w1)


def second_kernel(place, targets, near, early_stat, x0, x1, x2, x3, weight, out, logits, stat):
    logits[...] = near[...] + dot_t(weight[...], jnp.concatenate([x0[...], x1[...], x2[...], x3[...]], axis=0))
    sums = token_sums(place, wanted_of(place, targets, (2, 3)), logits)
    for i, total in enumerate(sums):
        for k in range(2):
            stat[pl.ds(place[3 + k] + 4 * i, 1), :] = early_stat[2 * i + k:2 * i + k + 1, :]
            stat[pl.ds(place[5 + k] + 4 * i, 1), :] = total[:, k * 128:(k + 1) * 128]
    for i in range(out.shape[0]):
        out[i] = stat[...]


def second_product(place, targets, near, early_stat, xs, weight, copies):
    vocab, depth = weight.shape
    inside = pl.BlockSpec(memory_space=pltpu.VMEM)
    return pl.pallas_call(
        second_kernel,
        in_specs=[scalars()] + [inside] * 8,
        out_specs=inside,
        out_shape=jax.ShapeDtypeStruct((copies, *early_stat.shape), jnp.float32),
        scratch_shapes=[pltpu.VMEM(near.shape, jnp.float32), pltpu.VMEM(early_stat.shape, jnp.float32)],
        compiler_params=params(VMEM_LIMIT),
        cost_estimate=pl.CostEstimate(flops=2 * vocab * 256 * depth, bytes_accessed=10 * 2**20, transcendentals=0),
        name="second_product",
    )(place, targets, near, early_stat, *xs, weight)


def join_kernel(parts, out):
    total = jnp.sum(parts[...], axis=0)
    for i in range(out.shape[0]):
        out[i] = total


def join(parts, copies):
    shape = (copies, *parts.shape[1:])
    return pl.pallas_call(
        join_kernel,
        in_specs=[whole(parts.shape)],
        out_specs=whole(shape),
        out_shape=jax.ShapeDtypeStruct(shape, jnp.float32),
        compiler_params=params(),
        name="join",
    )(parts)


def loss_kernel(place, count, live, parts, token_loss, mean_loss, loss):
    groups = parts.shape[1] // 2
    for core in range(2):
        total = parts[core]
        for i in range(core + 2, parts.shape[0], 2):
            total = total + parts[i]
        rows = slice(core * groups, (core + 1) * groups)
        loss[rows, :] = live[rows, :] * (jnp.log(total[:groups]) - total[groups:])
    mean_loss[0] = jnp.sum(loss[...]) / count[0]
    own = loss[pl.ds(place[0], 1), :]
    lane = lax.broadcasted_iota(jnp.int32, own.shape, 1)
    for i in range(token_loss.shape[0]):
        token_loss[i] = jnp.sum(jnp.where(lane == place[1] + i, own, 0.0))


def final_loss(place, count, live, parts, own_rows):
    return pl.pallas_call(
        loss_kernel,
        in_specs=[scalars(), scalars(), whole(live.shape), whole(parts.shape)],
        out_specs=[scalars(), scalars()],
        out_shape=[jax.ShapeDtypeStruct((own_rows,), jnp.float32), jax.ShapeDtypeStruct((1,), jnp.float32)],
        scratch_shapes=[pltpu.VMEM(live.shape, jnp.float32)],
        compiler_params=params(),
        name="final_loss",
    )(place, count, live, parts)


def in_hbm(value):
    return pltpu.with_memory_space_constraint(value, pltpu.HBM)


def exchange(value, axes):
    return lax.all_to_all(value, axes, 0, 0)


def body(hidden, norm_gain, head_weight, targets, lengths):
    own_rows = hidden.shape[0]
    vocab_rows = head_weight.shape[0]
    nx, nc = lax.axis_size("x"), lax.axis_size("c")
    plane = lax.axis_size(PLANE)
    x, c = lax.axis_index("x"), lax.axis_index("c")
    seat = lax.axis_index(PLANE)
    block = plane * own_rows

    def turn(value, k):
        return lax.ppermute(value, "x", [(i, (i + k) % nx) for i in range(nx)])

    wide, narrow = norm(hidden, norm_gain, plane, WIDE)
    mine = exchange(wide, PLANE).reshape(block, WIDE)
    other_weight = lax.ppermute(head_weight, "c", [(0, 1), (1, 0)])
    column = jnp.concatenate([narrow, turn(narrow, 1), turn(narrow, nx - 1), turn(narrow, 2)], axis=0)
    mixed = exchange(jnp.broadcast_to(column[None], (plane, *column.shape)), PLANE).reshape(nx * block, -1)
    low, high = mine[:block // 2], mine[block // 2:]
    up_low, down_high = turn(low, 1), turn(high, nx - 1)
    up_high, down_low = turn(high, 1), turn(low, nx - 1)
    far_low, far_high = turn(up_low, 1), turn(down_high, nx - 1)
    sources = [lax.rem(x + nx - k, nx) for k in (0, 1, nx - 1, 2)]
    first = ((x * nc + c) * plane + seat) * vocab_rows
    second = ((x * nc + 1 - c) * plane + seat) * vocab_rows
    place = jnp.stack([c, first, second, *sources]).astype(jnp.int32)
    ids = targets.reshape(nx * nc, block)
    shards = in_hbm(head_weight), in_hbm(other_weight)
    near, early, weight = first_product(place, ids, (low, high, up_low, up_high), mixed, *shards)
    stats = second_product(place, ids, near, early, (down_low, down_high, far_low, far_high), weight, plane)
    stats = join(exchange(stats, PLANE), nx * nc)
    stats = exchange(stats, ("x", "c"))
    position = jnp.arange(WINDOW, dtype=jnp.int32)
    live = (position[None, :] < lengths[:, None]).astype(jnp.float32).reshape(nx, nc, block)
    live = live.transpose(1, 0, 2).reshape(nx * nc, block)
    count = jnp.sum(lengths.astype(jnp.float32)).reshape(1)
    seat_of = jnp.stack([c * nx + x, seat * own_rows]).astype(jnp.int32)
    token_loss, mean_loss = final_loss(seat_of, count, live, stats, own_rows)
    return (token_loss, mean_loss.reshape(()))


def solution(mesh):
    split = Mesh(mesh.devices.reshape(4, 2, 8, 8), TOK_VOC)
    in_specs = (P(TOK_VOC, None), P(), P(TOK_VOC, None), P(), P())
    out_specs = (P(TOK_VOC), P())
    return jax.shard_map(body, mesh=split, in_specs=in_specs, out_specs=out_specs, check_vma=False)
```

```python
import jax
import jax.numpy as jnp
from jax import lax
from jax.experimental import pallas as pl
from jax.experimental.pallas import tpu as pltpu
from jax.sharding import Mesh
from jax.sharding import PartitionSpec as P

WINDOW = 32
TOK_VOC = ("x", "c", "z", "y")
PLANE = ("z", "y")
WIDE = 3584
STRIP = 64
CHUNKS = 2
VMEM_LIMIT = 12 * 2**20
WIDE_VMEM = 20 * 2**20


def params(limit=8 * 2**20):
    return pltpu.CompilerParams(vmem_limit_bytes=limit)


def whole(shape):
    return pl.BlockSpec(shape, lambda *_: (0,) * len(shape))


def scalars():
    return pl.BlockSpec(memory_space=pltpu.SMEM)


def dot_t(a, b):
    return lax.dot_general(a, b, (((1,), (1,)), ((), ())), preferred_element_type=jnp.float32)


def norm_kernel(hidden, gain, wide, narrow):
    values = hidden[...].astype(jnp.float32)
    meansq = jnp.mean(values * values, axis=1, keepdims=True)
    normed = (values * lax.rsqrt(meansq + 1e-06) * gain[...].reshape(1, -1)).astype(jnp.bfloat16)
    width = wide.shape[2]
    narrow[...] = normed[:, width:]
    for i in range(wide.shape[0]):
        wide[i] = normed[:, :width]


def norm(hidden, gain, copies, width):
    rows, depth = hidden.shape
    shapes = [(copies, rows, width), (rows, depth - width)]
    return pl.pallas_call(
        norm_kernel,
        in_specs=[whole(hidden.shape), whole(gain.shape)],
        out_specs=[whole(s) for s in shapes],
        out_shape=[jax.ShapeDtypeStruct(s, jnp.bfloat16) for s in shapes],
        compiler_params=params(),
        name="norm",
    )(in_hbm(hidden), in_hbm(gain))


def position(own_rows):
    x, c = lax.axis_index("x"), lax.axis_index("c")
    seat = lax.axis_index("z") * lax.axis_size("y") + lax.axis_index("y")
    return x, c, seat * own_rows


def sources(x):
    nx = lax.axis_size("x")
    return [lax.rem(x + nx - k, nx) for k in (0, 1, nx - 1, 2)]


def token_sums(targets, groups, logits):
    vocab, tokens = logits.shape
    shard = vocab // 2
    x, c, seat = position(1)
    nc, plane = lax.axis_size("c"), lax.axis_size(PLANE)
    starts = [((x * nc + core) * plane + seat) * shard for core in (c, 1 - c)]
    wanted = jnp.concatenate([targets[pl.ds(sources(x)[k] * nc + c, 1), :] for k in groups], axis=1)
    expsum = jnp.zeros((8, tokens), jnp.float32)
    picked = jnp.zeros((8, tokens), jnp.float32)
    column = lax.broadcasted_iota(jnp.int32, (STRIP, tokens), 0)
    for r in range(0, vocab, STRIP):
        half, offset = divmod(r, shard)
        capped = 30.0 * jnp.tanh(logits[r:r + STRIP, :] / 30.0)
        hit = jnp.where(column == wanted - (starts[half] + offset), capped, 0.0)
        expsum += jnp.sum(jnp.exp(capped).reshape(STRIP // 8, 8, tokens), axis=0)
        picked += jnp.sum(hit.reshape(STRIP // 8, 8, tokens), axis=0)
    return jnp.sum(expsum, axis=0, keepdims=True), jnp.sum(picked, axis=0, keepdims=True)


def fetch(shards, kept, sems, starts, width):
    vocab = shards[0].shape[0]
    copies = []
    for i, start in enumerate(starts):
        pair = []
        for j, shard in enumerate(shards):
            source = shard.at[:, start:start + width]
            target = kept.at[j * vocab:(j + 1) * vocab, start:start + width]
            pair.append(pltpu.make_async_copy(source, target, sems.at[2 * i + j]))
            pair[-1].start()
        copies.append(pair)
    return copies


def first_kernel(
    lengths, targets, x0, x1, x2, x3, mixed, w0, w1, late, stat, live, kept, rows, logits, narrow_w, sems
):
    wide = x0.shape[1]
    tokens = mixed.shape[0]
    groups = tokens // 128
    early = logits.shape[1]
    half = tokens // 2
    vocab = w0.shape[0]
    copies = [
        pltpu.make_async_copy(w.at[:, wide:], narrow_w.at[j * vocab:(j + 1) * vocab, :], sems.at[2 * CHUNKS + j])
        for j, w in enumerate((w0, w1))
    ]
    for copy in copies:
        copy.start()
    width = wide // CHUNKS
    others = fetch((w0, w1), kept, sems, [i * width for i in range(CHUNKS)], width)
    lane = lax.broadcasted_iota(jnp.int32, (1, 128), 1)
    count = 0
    for core in range(2):
        for k in range(groups):
            length = jnp.zeros((1, 128), jnp.int32)
            for j in range(128 // WINDOW):
                here = lengths[(k * 2 + core) * (128 // WINDOW) + j]
                count = count + here
                length = jnp.where(lane // WINDOW == j, here, length)
            i = core * groups + k
            live[i:i + 1, :] = jnp.where(lane % WINDOW < length, 1.0, 0.0)
    live[2 * groups:, :] = jnp.full((2 * groups, 128), count, jnp.int32).astype(jnp.float32)
    row = lax.broadcasted_iota(jnp.int32, (half, half), 0)
    col = lax.broadcasted_iota(jnp.int32, (half, half), 1)
    inner = row & 63
    pick = (inner >> 1) * (2 * groups) + (row >> 6) * 2 + (inner & 1)
    chosen = jnp.where(col == pick, 1.0, 0.0).astype(jnp.bfloat16)
    for h in range(2):
        part = jnp.dot(chosen, mixed[h * half:(h + 1) * half, :], preferred_element_type=jnp.float32)
        for k in range(groups):
            rows[k * 128 + h * 64:k * 128 + h * 64 + 64, :] = part[k * 64:(k + 1) * 64].astype(jnp.bfloat16)
    for copy in copies:
        copy.wait()
    late[...] = dot_t(narrow_w[...], rows[early:, :])
    logits[...] = dot_t(narrow_w[...], rows[:early, :])
    for i in range(CHUNKS):
        for copy in others[i]:
            copy.wait()
        cols = slice(i * width, (i + 1) * width)
        x = jnp.concatenate([x0[:, cols], x1[:, cols], x2[:, cols], x3[:, cols]], axis=0)
        logits[...] += dot_t(kept[:, cols], x)
    for i, total in enumerate(token_sums(targets, (0, 1), logits)):
        for k in range(2):
            stat[2 * i + k:2 * i + k + 1, :] = total[:, k * 128:(k + 1) * 128]


INSIDE = pl.BlockSpec(memory_space=pltpu.VMEM)


def first_product(lengths, targets, xs, mixed, w0, w1):
    vocab, depth = 2 * w0.shape[0], w0.shape[1]
    tokens, narrow = mixed.shape
    early = sum(x.shape[0] for x in xs)
    return pl.pallas_call(
        first_kernel,
        in_specs=[scalars()] + [INSIDE] * 6 + [pl.BlockSpec(memory_space=pltpu.HBM)] * 2,
        out_specs=[INSIDE] * 4,
        out_shape=[
            jax.ShapeDtypeStruct((vocab, tokens - early), jnp.float32),
            jax.ShapeDtypeStruct((8, 128), jnp.float32),
            jax.ShapeDtypeStruct((16, 128), jnp.float32),
            jax.ShapeDtypeStruct((vocab, depth - narrow), w0.dtype),
        ],
        scratch_shapes=[
            pltpu.VMEM((tokens, narrow), jnp.bfloat16),
            pltpu.VMEM((vocab, early), jnp.float32),
            pltpu.VMEM((vocab, narrow), w0.dtype),
            pltpu.SemaphoreType.DMA((2 * CHUNKS + 2,)),
        ],
        compiler_params=params(WIDE_VMEM),
        cost_estimate=pl.CostEstimate(flops=vocab * tokens * depth, bytes_accessed=14 * 2**20, transcendentals=0),
        name="first_product",
    )(lengths, targets, *xs, mixed, w0, w1)


def last_kernel(targets, late, early_stat, x0, x1, x2, x3, weight, out, logits, stat):
    logits[...] = late[...] + dot_t(weight[...], jnp.concatenate([x0[...], x1[...], x2[...], x3[...]], axis=0))
    origin = sources(lax.axis_index("x"))
    for i, total in enumerate(token_sums(targets, (2, 3), logits)):
        for k in range(2):
            stat[pl.ds(origin[k] + 4 * i, 1), :] = early_stat[2 * i + k:2 * i + k + 1, :]
            stat[pl.ds(origin[2 + k] + 4 * i, 1), :] = total[:, k * 128:(k + 1) * 128]
    for i in range(out.shape[0]):
        out[i] = stat[...]


def last_product(targets, late, early_stat, xs, weight, copies):
    vocab, depth = weight.shape
    return pl.pallas_call(
        last_kernel,
        in_specs=[INSIDE] * 8,
        out_specs=INSIDE,
        out_shape=jax.ShapeDtypeStruct((copies, *early_stat.shape), jnp.float32),
        scratch_shapes=[pltpu.VMEM(late.shape, jnp.float32), pltpu.VMEM(early_stat.shape, jnp.float32)],
        compiler_params=params(VMEM_LIMIT),
        cost_estimate=pl.CostEstimate(flops=2 * vocab * 256 * depth, bytes_accessed=10 * 2**20, transcendentals=0),
        name="last_product",
    )(targets, late, early_stat, *xs, weight)


def join_kernel(parts, out):
    total = jnp.sum(parts[...], axis=0)
    for i in range(out.shape[0]):
        out[i] = total


def join(parts, copies):
    return pl.pallas_call(
        join_kernel,
        in_specs=[INSIDE],
        out_specs=INSIDE,
        out_shape=jax.ShapeDtypeStruct((copies, *parts.shape[1:]), jnp.float32),
        compiler_params=params(),
        name="join",
    )(parts)


def loss_kernel(live, parts, token_loss, mean_loss, loss):
    groups = parts.shape[1] // 2
    for core in range(2):
        total = parts[core]
        for i in range(core + 2, parts.shape[0], 2):
            total = total + parts[i]
        rows = slice(core * groups, (core + 1) * groups)
        loss[rows, :] = live[rows, :] * (jnp.log(total[:groups]) - total[groups:])
    mean_loss[0] = jnp.sum(loss[...]) / live[2 * groups, 0]
    own_rows = token_loss.shape[0]
    x, c, seat = position(own_rows)
    own = loss[pl.ds(c * groups + x, 1), :]
    lane = lax.broadcasted_iota(jnp.int32, own.shape, 1)
    for i in range(own_rows):
        token_loss[i] = jnp.sum(jnp.where(lane == seat + i, own, 0.0))


def final_loss(live, parts, own_rows):
    return pl.pallas_call(
        loss_kernel,
        in_specs=[INSIDE] * 2,
        out_specs=[scalars(), scalars()],
        out_shape=[jax.ShapeDtypeStruct((own_rows,), jnp.float32), jax.ShapeDtypeStruct((1,), jnp.float32)],
        scratch_shapes=[pltpu.VMEM(parts.shape[1:], jnp.float32)],
        compiler_params=params(),
        name="final_loss",
    )(live, parts)


def in_hbm(value):
    return pltpu.with_memory_space_constraint(value, pltpu.HBM)


def exchange(value, axes):
    return lax.all_to_all(value, axes, 0, 0)


def body(hidden, norm_gain, head_weight, targets, lengths):
    own_rows = hidden.shape[0]
    nx, nc = lax.axis_size("x"), lax.axis_size("c")
    plane = lax.axis_size(PLANE)
    block = plane * own_rows

    def turn(value, k):
        return lax.ppermute(value, "x", [(i, (i + k) % nx) for i in range(nx)])

    wide, narrow = norm(hidden, norm_gain, plane, WIDE)
    mine = exchange(wide, PLANE).reshape(block, WIDE)
    other_weight = lax.ppermute(head_weight, "c", [(0, 1), (1, 0)])
    column = jnp.concatenate([narrow, turn(narrow, 1), turn(narrow, nx - 1), turn(narrow, 2)], axis=0)
    mixed = exchange(jnp.broadcast_to(column[None], (plane, *column.shape)), PLANE).reshape(nx * block, -1)
    low, high = mine[:block // 2], mine[block // 2:]
    up_low, down_high = turn(low, 1), turn(high, nx - 1)
    up_high, down_low = turn(high, 1), turn(low, nx - 1)
    far_low, far_high = turn(up_low, 1), turn(down_high, nx - 1)
    ids = targets.reshape(nx * nc, block)
    shards = in_hbm(head_weight), in_hbm(other_weight)
    late, early, live, wide_w = first_product(lengths, ids, (low, high, up_low, up_high), mixed, *shards)
    stats = last_product(ids, late, early, (down_low, down_high, far_low, far_high), wide_w, plane)
    stats = join(exchange(stats, PLANE), nx * nc)
    stats = exchange(stats, ("x", "c"))
    token_loss, mean_loss = final_loss(live, stats, own_rows)
    return (token_loss, mean_loss.reshape(()))


def solution(mesh):
    split = Mesh(mesh.devices.reshape(4, 2, 8, 8), TOK_VOC)
    in_specs = (P(TOK_VOC, None), P(), P(TOK_VOC, None), P(), P())
    out_specs = (P(TOK_VOC), P())
    return jax.shard_map(body, mesh=split, in_specs=in_specs, out_specs=out_specs, check_vma=False)
```

```python
import jax
import jax.numpy as jnp
from jax import lax
from jax.experimental import pallas as pl
from jax.experimental.pallas import tpu as pltpu
from jax.sharding import Mesh
from jax.sharding import PartitionSpec as P

WINDOW = 32
TOK_VOC = ("x", "c", "z", "y")
PLANE = ("z", "y")
WIDE = 3584
STRIP = 64
CHUNKS = 2
VMEM_LIMIT = 12 * 2**20
WIDE_VMEM = 20 * 2**20


def params(limit=8 * 2**20):
    return pltpu.CompilerParams(vmem_limit_bytes=limit)


def whole(shape):
    return pl.BlockSpec(shape, lambda *_: (0,) * len(shape))


def scalars():
    return pl.BlockSpec(memory_space=pltpu.SMEM)


def dot_t(a, b):
    return lax.dot_general(a, b, (((1,), (1,)), ((), ())), preferred_element_type=jnp.float32)


def norm_kernel(hidden, gain, wide, narrow):
    values = hidden[...].astype(jnp.float32)
    meansq = jnp.mean(values * values, axis=1, keepdims=True)
    normed = (values * lax.rsqrt(meansq + 1e-06) * gain[...].reshape(1, -1)).astype(jnp.bfloat16)
    width = wide.shape[2]
    narrow[...] = normed[:, width:]
    for i in range(wide.shape[0]):
        wide[i] = normed[:, :width]


def norm(hidden, gain, copies, width):
    rows, depth = hidden.shape
    shapes = [(copies, rows, width), (rows, depth - width)]
    return pl.pallas_call(
        norm_kernel,
        in_specs=[whole(hidden.shape), whole(gain.shape)],
        out_specs=[whole(s) for s in shapes],
        out_shape=[jax.ShapeDtypeStruct(s, jnp.bfloat16) for s in shapes],
        compiler_params=params(),
        name="norm",
    )(in_hbm(hidden), in_hbm(gain))


def position(own_rows):
    x, c = lax.axis_index("x"), lax.axis_index("c")
    seat = lax.axis_index("z") * lax.axis_size("y") + lax.axis_index("y")
    return x, c, seat * own_rows


def sources(x):
    nx = lax.axis_size("x")
    return [lax.rem(x + nx - k, nx) for k in (0, 1, nx - 1, 2)]


def token_sums(targets, groups, logits):
    vocab, tokens = logits.shape
    shard = vocab // 2
    x, c, seat = position(1)
    nc, plane = lax.axis_size("c"), lax.axis_size(PLANE)
    starts = [((x * nc + core) * plane + seat) * shard for core in (c, 1 - c)]
    wanted = jnp.concatenate([targets[pl.ds(sources(x)[k] * nc + c, 1), :] for k in groups], axis=1)
    expsum = jnp.zeros((8, tokens), jnp.float32)
    picked = jnp.zeros((8, tokens), jnp.float32)
    column = lax.broadcasted_iota(jnp.int32, (STRIP, tokens), 0)
    for r in range(0, vocab, STRIP):
        half, offset = divmod(r, shard)
        capped = 30.0 * jnp.tanh(logits[r:r + STRIP, :] / 30.0)
        hit = jnp.where(column == wanted - (starts[half] + offset), capped, 0.0)
        expsum += jnp.sum(jnp.exp(capped).reshape(STRIP // 8, 8, tokens), axis=0)
        picked += jnp.sum(hit.reshape(STRIP // 8, 8, tokens), axis=0)
    return jnp.sum(expsum, axis=0, keepdims=True), jnp.sum(picked, axis=0, keepdims=True)


def fetch(shards, kept, sems, starts, width):
    vocab = shards[0].shape[0]
    copies = []
    for i, start in enumerate(starts):
        pair = []
        for j, shard in enumerate(shards):
            source = shard.at[:, start:start + width]
            target = kept.at[j * vocab:(j + 1) * vocab, start:start + width]
            pair.append(pltpu.make_async_copy(source, target, sems.at[2 * i + j]))
            pair[-1].start()
        copies.append(pair)
    return copies


def early_kernel(lengths, x0, x1, x2, x3, w0, w1, logits, live, weight, sems):
    wide = x0.shape[1]
    width = wide // CHUNKS
    copies = fetch((w0, w1), weight, sems, [i * width for i in range(CHUNKS)], width)
    lane = lax.broadcasted_iota(jnp.int32, (1, 128), 1)
    groups = live.shape[0] // 4
    count = 0
    for core in range(2):
        for k in range(groups):
            length = jnp.zeros((1, 128), jnp.int32)
            for j in range(128 // WINDOW):
                here = lengths[(k * 2 + core) * (128 // WINDOW) + j]
                count = count + here
                length = jnp.where(lane // WINDOW == j, here, length)
            i = core * groups + k
            live[i:i + 1, :] = jnp.where(lane % WINDOW < length, 1.0, 0.0)
    live[2 * groups:, :] = jnp.full((2 * groups, 128), count, jnp.int32).astype(jnp.float32)
    for i in range(CHUNKS):
        for copy in copies[i]:
            copy.wait()
        cols = slice(i * width, (i + 1) * width)
        x = jnp.concatenate([x0[:, cols], x1[:, cols], x2[:, cols], x3[:, cols]], axis=0)
        part = dot_t(weight[:, cols], x)
        if i == 0:
            logits[...] = part
        else:
            logits[...] += part


INSIDE = pl.BlockSpec(memory_space=pltpu.VMEM)
OUTSIDE = pl.BlockSpec(memory_space=pltpu.HBM)


def early_product(lengths, xs, w0, w1):
    vocab = 2 * w0.shape[0]
    wide = xs[0].shape[1]
    tokens = sum(x.shape[0] for x in xs)
    return pl.pallas_call(
        early_kernel,
        in_specs=[scalars()] + [INSIDE] * 4 + [OUTSIDE] * 2,
        out_specs=[INSIDE] * 2,
        out_shape=[
            jax.ShapeDtypeStruct((vocab, tokens), jnp.float32),
            jax.ShapeDtypeStruct((16, 128), jnp.float32),
        ],
        scratch_shapes=[pltpu.VMEM((vocab, wide), w0.dtype), pltpu.SemaphoreType.DMA((2 * CHUNKS,))],
        compiler_params=params(WIDE_VMEM),
        cost_estimate=pl.CostEstimate(flops=2 * vocab * tokens * wide, bytes_accessed=10 * 2**20, transcendentals=0),
        name="early_product",
    )(lengths, *xs, w0, w1)


def mixed_kernel(targets, near, mixed, w0, w1, late, stat, kept, rows, logits, narrow_w, sems):
    tokens = mixed.shape[0]
    groups = tokens // 128
    early = logits.shape[1]
    half = tokens // 2
    vocab = w0.shape[0]
    wide = kept.shape[1]
    copies = [
        pltpu.make_async_copy(w.at[:, wide:], narrow_w.at[j * vocab:(j + 1) * vocab, :], sems.at[2 + j])
        for j, w in enumerate((w0, w1))
    ]
    for copy in copies:
        copy.start()
    others = fetch((w0, w1), kept, sems, [0], wide)
    row = lax.broadcasted_iota(jnp.int32, (half, half), 0)
    col = lax.broadcasted_iota(jnp.int32, (half, half), 1)
    inner = row & 63
    pick = (inner >> 1) * (2 * groups) + (row >> 6) * 2 + (inner & 1)
    chosen = jnp.where(col == pick, 1.0, 0.0).astype(jnp.bfloat16)
    for h in range(2):
        part = jnp.dot(chosen, mixed[h * half:(h + 1) * half, :], preferred_element_type=jnp.float32)
        for k in range(groups):
            rows[k * 128 + h * 64:k * 128 + h * 64 + 64, :] = part[k * 64:(k + 1) * 64].astype(jnp.bfloat16)
    for copy in copies:
        copy.wait()
    late[...] = dot_t(narrow_w[...], rows[early:, :])
    logits[...] = near[...] + dot_t(narrow_w[...], rows[:early, :])
    for i, total in enumerate(token_sums(targets, (0, 1), logits)):
        for k in range(2):
            stat[2 * i + k:2 * i + k + 1, :] = total[:, k * 128:(k + 1) * 128]
    for copy in others[0]:
        copy.wait()


def mixed_product(targets, near, mixed, w0, w1):
    vocab, depth = 2 * w0.shape[0], w0.shape[1]
    tokens, narrow = mixed.shape
    early = near.shape[1]
    return pl.pallas_call(
        mixed_kernel,
        in_specs=[INSIDE] * 3 + [OUTSIDE] * 2,
        out_specs=[INSIDE] * 3,
        out_shape=[
            jax.ShapeDtypeStruct((vocab, tokens - early), jnp.float32),
            jax.ShapeDtypeStruct((8, 128), jnp.float32),
            jax.ShapeDtypeStruct((vocab, depth - narrow), w0.dtype),
        ],
        scratch_shapes=[
            pltpu.VMEM((tokens, narrow), jnp.bfloat16),
            pltpu.VMEM((vocab, early), jnp.float32),
            pltpu.VMEM((vocab, narrow), w0.dtype),
            pltpu.SemaphoreType.DMA((4,)),
        ],
        compiler_params=params(WIDE_VMEM),
        cost_estimate=pl.CostEstimate(flops=2 * vocab * tokens * narrow, bytes_accessed=12 * 2**20, transcendentals=0),
        name="mixed_product",
    )(targets, near, mixed, w0, w1)


def last_kernel(targets, late, early_stat, x0, x1, x2, x3, weight, out, logits, stat):
    logits[...] = late[...] + dot_t(weight[...], jnp.concatenate([x0[...], x1[...], x2[...], x3[...]], axis=0))
    origin = sources(lax.axis_index("x"))
    for i, total in enumerate(token_sums(targets, (2, 3), logits)):
        for k in range(2):
            stat[pl.ds(origin[k] + 4 * i, 1), :] = early_stat[2 * i + k:2 * i + k + 1, :]
            stat[pl.ds(origin[2 + k] + 4 * i, 1), :] = total[:, k * 128:(k + 1) * 128]
    for i in range(out.shape[0]):
        out[i] = stat[...]


def last_product(targets, late, early_stat, xs, weight, copies):
    vocab, depth = weight.shape
    return pl.pallas_call(
        last_kernel,
        in_specs=[INSIDE] * 8,
        out_specs=INSIDE,
        out_shape=jax.ShapeDtypeStruct((copies, *early_stat.shape), jnp.float32),
        scratch_shapes=[pltpu.VMEM(late.shape, jnp.float32), pltpu.VMEM(early_stat.shape, jnp.float32)],
        compiler_params=params(VMEM_LIMIT),
        cost_estimate=pl.CostEstimate(flops=2 * vocab * 256 * depth, bytes_accessed=10 * 2**20, transcendentals=0),
        name="last_product",
    )(targets, late, early_stat, *xs, weight)


def join_kernel(parts, out):
    total = jnp.sum(parts[...], axis=0)
    for i in range(out.shape[0]):
        out[i] = total


def join(parts, copies):
    return pl.pallas_call(
        join_kernel,
        in_specs=[INSIDE],
        out_specs=INSIDE,
        out_shape=jax.ShapeDtypeStruct((copies, *parts.shape[1:]), jnp.float32),
        compiler_params=params(),
        name="join",
    )(parts)


def loss_kernel(live, parts, token_loss, mean_loss, loss):
    groups = parts.shape[1] // 2
    for core in range(2):
        total = jnp.sum(parts[core * parts.shape[0] // 2:(core + 1) * parts.shape[0] // 2], axis=0)
        rows = slice(core * groups, (core + 1) * groups)
        loss[rows, :] = live[rows, :] * (jnp.log(total[:groups]) - total[groups:])
    mean_loss[0] = jnp.sum(loss[...]) / live[2 * groups, 0]
    own_rows = token_loss.shape[0]
    x, c, seat = position(own_rows)
    own = loss[pl.ds(c * groups + x, 1), :]
    lane = lax.broadcasted_iota(jnp.int32, own.shape, 1)
    for i in range(own_rows):
        token_loss[i] = jnp.sum(jnp.where(lane == seat + i, own, 0.0))


def final_loss(live, parts, own_rows):
    return pl.pallas_call(
        loss_kernel,
        in_specs=[INSIDE] * 2,
        out_specs=[scalars(), scalars()],
        out_shape=[jax.ShapeDtypeStruct((own_rows,), jnp.float32), jax.ShapeDtypeStruct((1,), jnp.float32)],
        scratch_shapes=[pltpu.VMEM(parts.shape[1:], jnp.float32)],
        compiler_params=params(),
        name="final_loss",
    )(live, parts)


def in_hbm(value):
    return pltpu.with_memory_space_constraint(value, pltpu.HBM)


def exchange(value, axes):
    return lax.all_to_all(value, axes, 0, 0)


def body(hidden, norm_gain, head_weight, targets, lengths):
    own_rows = hidden.shape[0]
    nx, nc = lax.axis_size("x"), lax.axis_size("c")
    plane = lax.axis_size(PLANE)
    block = plane * own_rows

    def turn(value, k):
        return lax.ppermute(value, "x", [(i, (i + k) % nx) for i in range(nx)])

    wide, narrow = norm(hidden, norm_gain, plane, WIDE)
    mine = exchange(wide, PLANE).reshape(block, WIDE)
    other_weight = lax.ppermute(head_weight, "c", [(0, 1), (1, 0)])
    column = jnp.concatenate([narrow, turn(narrow, 1), turn(narrow, nx - 1), turn(narrow, 2)], axis=0)
    mixed = exchange(jnp.broadcast_to(column[None], (plane, *column.shape)), PLANE).reshape(nx * block, -1)
    low, high = mine[:block // 2], mine[block // 2:]
    up_low, down_high = turn(low, 1), turn(high, nx - 1)
    up_high, down_low = turn(high, 1), turn(low, nx - 1)
    far_low, far_high = turn(up_low, 1), turn(down_high, nx - 1)
    ids = targets.reshape(nx * nc, block)
    shards = in_hbm(head_weight), in_hbm(other_weight)
    near, live = early_product(lengths, (low, high, up_low, up_high), *shards)
    late, early, wide_w = mixed_product(ids, near, mixed, *shards)
    stats = last_product(ids, late, early, (down_low, down_high, far_low, far_high), wide_w, lax.axis_size(("x", "z")))
    stats = join(exchange(stats, ("x", "z")), lax.axis_size(("c", "y")))
    stats = exchange(stats, ("c", "y"))
    token_loss, mean_loss = final_loss(live, stats, own_rows)
    return (token_loss, mean_loss.reshape(()))


def solution(mesh):
    split = Mesh(mesh.devices.reshape(4, 2, 8, 8), TOK_VOC)
    in_specs = (P(TOK_VOC, None), P(), P(TOK_VOC, None), P(), P())
    out_specs = (P(TOK_VOC), P())
    return jax.shard_map(body, mesh=split, in_specs=in_specs, out_specs=out_specs, check_vma=False)
```

```python
import jax
import jax.numpy as jnp
from jax import lax
from jax.experimental import pallas as pl
from jax.experimental.pallas import tpu as pltpu
from jax.sharding import Mesh
from jax.sharding import PartitionSpec as P

WINDOW = 32
TOK_VOC = ("x", "c", "z", "y")
PLANE = ("z", "y")
WIDE = 3712
STRIP = 64
VMEM_LIMIT = 12 * 2**20
WIDE_VMEM = 20 * 2**20


def params(limit=8 * 2**20):
    return pltpu.CompilerParams(vmem_limit_bytes=limit)


def whole(shape):
    return pl.BlockSpec(shape, lambda *_: (0,) * len(shape))


def scalars():
    return pl.BlockSpec(memory_space=pltpu.SMEM)


def dot_t(a, b):
    return lax.dot_general(a, b, (((1,), (1,)), ((), ())), preferred_element_type=jnp.float32)


def norm_kernel(hidden, gain, wide, narrow):
    values = hidden[...].astype(jnp.float32)
    meansq = jnp.mean(values * values, axis=1, keepdims=True)
    normed = (values * lax.rsqrt(meansq + 1e-06) * gain[...].reshape(1, -1)).astype(jnp.bfloat16)
    width = wide.shape[2]
    narrow[...] = normed[:, width:]
    for i in range(wide.shape[0]):
        wide[i] = normed[:, :width]


def norm(hidden, gain, copies, width):
    rows, depth = hidden.shape
    shapes = [(copies, rows, width), (rows, depth - width)]
    return pl.pallas_call(
        norm_kernel,
        in_specs=[whole(hidden.shape), whole(gain.shape)],
        out_specs=[whole(s) for s in shapes],
        out_shape=[jax.ShapeDtypeStruct(s, jnp.bfloat16) for s in shapes],
        compiler_params=params(),
        name="norm",
    )(in_hbm(hidden), in_hbm(gain))


def position(own_rows):
    x, c = lax.axis_index("x"), lax.axis_index("c")
    seat = lax.axis_index("z") * lax.axis_size("y") + lax.axis_index("y")
    return x, c, seat * own_rows


def sources(x):
    nx = lax.axis_size("x")
    return [lax.rem(x + nx - k, nx) for k in (0, 1, nx - 1, 2)]


def token_sums(targets, groups, logits):
    vocab, tokens = logits.shape
    shard = vocab // 2
    x, c, seat = position(1)
    nc, plane = lax.axis_size("c"), lax.axis_size(PLANE)
    starts = [((x * nc + core) * plane + seat) * shard for core in (c, 1 - c)]
    wanted = jnp.concatenate([targets[pl.ds(sources(x)[k] * nc + c, 1), :] for k in groups], axis=1)
    expsum = jnp.zeros((8, tokens), jnp.float32)
    picked = jnp.zeros((8, tokens), jnp.float32)
    column = lax.broadcasted_iota(jnp.int32, (STRIP, tokens), 0)
    for r in range(0, vocab, STRIP):
        half, offset = divmod(r, shard)
        capped = 30.0 * jnp.tanh(logits[r:r + STRIP, :] / 30.0)
        hit = jnp.where(column == wanted - (starts[half] + offset), capped, 0.0)
        expsum += jnp.sum(jnp.exp(capped).reshape(STRIP // 8, 8, tokens), axis=0)
        picked += jnp.sum(hit.reshape(STRIP // 8, 8, tokens), axis=0)
    return jnp.sum(expsum, axis=0, keepdims=True), jnp.sum(picked, axis=0, keepdims=True)


def fetch(shards, kept, sems, spans):
    vocab = shards[0].shape[0]
    copies = []
    for i, (start, stop) in enumerate(spans):
        pair = []
        for j, shard in enumerate(shards):
            source = shard.at[:, start:stop]
            target = kept.at[j * vocab:(j + 1) * vocab, start:stop]
            pair.append(pltpu.make_async_copy(source, target, sems.at[2 * i + j]))
            pair[-1].start()
        copies.append(pair)
    return copies


def early_kernel(lengths, x0, x1, x2, x3, w0, w1, logits, live, weight, sems):
    wide = x0.shape[1]
    cut = wide // 256 * 128
    spans = ((0, cut), (cut, wide))
    copies = fetch((w0, w1), weight, sems, spans)
    lane = lax.broadcasted_iota(jnp.int32, (1, 128), 1)
    groups = live.shape[0] // 4
    count = 0
    for core in range(2):
        for k in range(groups):
            length = jnp.zeros((1, 128), jnp.int32)
            for j in range(128 // WINDOW):
                here = lengths[(k * 2 + core) * (128 // WINDOW) + j]
                count = count + here
                length = jnp.where(lane // WINDOW == j, here, length)
            i = core * groups + k
            live[i:i + 1, :] = jnp.where(lane % WINDOW < length, 1.0, 0.0)
    live[2 * groups:, :] = jnp.full((2 * groups, 128), count, jnp.int32).astype(jnp.float32)
    for i, span in enumerate(spans):
        for copy in copies[i]:
            copy.wait()
        cols = slice(*span)
        x = jnp.concatenate([x0[:, cols], x1[:, cols], x2[:, cols], x3[:, cols]], axis=0)
        part = dot_t(weight[:, cols], x)
        if i == 0:
            logits[...] = part
        else:
            logits[...] += part


INSIDE = pl.BlockSpec(memory_space=pltpu.VMEM)
OUTSIDE = pl.BlockSpec(memory_space=pltpu.HBM)


def early_product(lengths, xs, w0, w1):
    vocab = 2 * w0.shape[0]
    wide = xs[0].shape[1]
    tokens = sum(x.shape[0] for x in xs)
    return pl.pallas_call(
        early_kernel,
        in_specs=[scalars()] + [INSIDE] * 4 + [OUTSIDE] * 2,
        out_specs=[INSIDE] * 2,
        out_shape=[
            jax.ShapeDtypeStruct((vocab, tokens), jnp.float32),
            jax.ShapeDtypeStruct((16, 128), jnp.float32),
        ],
        scratch_shapes=[pltpu.VMEM((vocab, wide), w0.dtype), pltpu.SemaphoreType.DMA((4,))],
        compiler_params=params(WIDE_VMEM),
        cost_estimate=pl.CostEstimate(flops=2 * vocab * tokens * wide, bytes_accessed=10 * 2**20, transcendentals=0),
        name="early_product",
    )(lengths, *xs, w0, w1)


def mixed_kernel(targets, near, mixed, w0, w1, late, stat, kept, rows, logits, narrow_w, sems):
    tokens = mixed.shape[0]
    groups = tokens // 128
    early = logits.shape[1]
    half = tokens // 2
    vocab = w0.shape[0]
    wide = kept.shape[1]
    copies = [
        pltpu.make_async_copy(w.at[:, wide:], narrow_w.at[j * vocab:(j + 1) * vocab, :], sems.at[2 + j])
        for j, w in enumerate((w0, w1))
    ]
    for copy in copies:
        copy.start()
    others = fetch((w0, w1), kept, sems, ((0, wide),))
    row = lax.broadcasted_iota(jnp.int32, (half, half), 0)
    col = lax.broadcasted_iota(jnp.int32, (half, half), 1)
    inner = row & 63
    pick = (inner >> 1) * (2 * groups) + (row >> 6) * 2 + (inner & 1)
    chosen = jnp.where(col == pick, 1.0, 0.0).astype(jnp.bfloat16)
    for h in range(2):
        part = jnp.dot(chosen, mixed[h * half:(h + 1) * half, :], preferred_element_type=jnp.float32)
        for k in range(groups):
            rows[k * 128 + h * 64:k * 128 + h * 64 + 64, :] = part[k * 64:(k + 1) * 64].astype(jnp.bfloat16)
    for copy in copies:
        copy.wait()
    late[...] = dot_t(narrow_w[...], rows[early:, :])
    logits[...] = near[...] + dot_t(narrow_w[...], rows[:early, :])
    for i, total in enumerate(token_sums(targets, (0, 1), logits)):
        for k in range(2):
            stat[2 * i + k:2 * i + k + 1, :] = total[:, k * 128:(k + 1) * 128]
    for copy in others[0]:
        copy.wait()


def mixed_product(targets, near, mixed, w0, w1):
    vocab, depth = 2 * w0.shape[0], w0.shape[1]
    tokens, narrow = mixed.shape
    early = near.shape[1]
    return pl.pallas_call(
        mixed_kernel,
        in_specs=[INSIDE] * 3 + [OUTSIDE] * 2,
        out_specs=[INSIDE] * 3,
        out_shape=[
            jax.ShapeDtypeStruct((vocab, tokens - early), jnp.float32),
            jax.ShapeDtypeStruct((8, 128), jnp.float32),
            jax.ShapeDtypeStruct((vocab, depth - narrow), w0.dtype),
        ],
        scratch_shapes=[
            pltpu.VMEM((tokens, narrow), jnp.bfloat16),
            pltpu.VMEM((vocab, early), jnp.float32),
            pltpu.VMEM((vocab, narrow), w0.dtype),
            pltpu.SemaphoreType.DMA((4,)),
        ],
        compiler_params=params(WIDE_VMEM),
        cost_estimate=pl.CostEstimate(flops=2 * vocab * tokens * narrow, bytes_accessed=12 * 2**20, transcendentals=0),
        name="mixed_product",
    )(targets, near, mixed, w0, w1)


def last_kernel(targets, late, early_stat, x0, x1, x2, x3, weight, out, logits, stat):
    logits[...] = late[...] + dot_t(weight[...], jnp.concatenate([x0[...], x1[...], x2[...], x3[...]], axis=0))
    origin = sources(lax.axis_index("x"))
    for i, total in enumerate(token_sums(targets, (2, 3), logits)):
        for k in range(2):
            stat[pl.ds(origin[k] + 4 * i, 1), :] = early_stat[2 * i + k:2 * i + k + 1, :]
            stat[pl.ds(origin[2 + k] + 4 * i, 1), :] = total[:, k * 128:(k + 1) * 128]
    for i in range(out.shape[0]):
        out[i] = stat[...]


def last_product(targets, late, early_stat, xs, weight, copies):
    vocab, depth = weight.shape
    return pl.pallas_call(
        last_kernel,
        in_specs=[INSIDE] * 8,
        out_specs=INSIDE,
        out_shape=jax.ShapeDtypeStruct((copies, *early_stat.shape), jnp.float32),
        scratch_shapes=[pltpu.VMEM(late.shape, jnp.float32), pltpu.VMEM(early_stat.shape, jnp.float32)],
        compiler_params=params(VMEM_LIMIT),
        cost_estimate=pl.CostEstimate(flops=2 * vocab * 256 * depth, bytes_accessed=10 * 2**20, transcendentals=0),
        name="last_product",
    )(targets, late, early_stat, *xs, weight)


def join_kernel(parts, out):
    total = jnp.sum(parts[...], axis=0)
    for i in range(out.shape[0]):
        out[i] = total


def join(parts, copies):
    return pl.pallas_call(
        join_kernel,
        in_specs=[INSIDE],
        out_specs=INSIDE,
        out_shape=jax.ShapeDtypeStruct((copies, *parts.shape[1:]), jnp.float32),
        compiler_params=params(),
        name="join",
    )(parts)


def loss_kernel(live, parts, token_loss, mean_loss, loss):
    groups = parts.shape[1] // 2
    for core in range(2):
        total = jnp.sum(parts[core * parts.shape[0] // 2:(core + 1) * parts.shape[0] // 2], axis=0)
        rows = slice(core * groups, (core + 1) * groups)
        loss[rows, :] = live[rows, :] * (jnp.log(total[:groups]) - total[groups:])
    mean_loss[0] = jnp.sum(loss[...]) / live[2 * groups, 0]
    own_rows = token_loss.shape[0]
    x, c, seat = position(own_rows)
    own = loss[pl.ds(c * groups + x, 1), :]
    lane = lax.broadcasted_iota(jnp.int32, own.shape, 1)
    for i in range(own_rows):
        token_loss[i] = jnp.sum(jnp.where(lane == seat + i, own, 0.0))


def final_loss(live, parts, own_rows):
    return pl.pallas_call(
        loss_kernel,
        in_specs=[INSIDE] * 2,
        out_specs=[scalars(), scalars()],
        out_shape=[jax.ShapeDtypeStruct((own_rows,), jnp.float32), jax.ShapeDtypeStruct((1,), jnp.float32)],
        scratch_shapes=[pltpu.VMEM(parts.shape[1:], jnp.float32)],
        compiler_params=params(),
        name="final_loss",
    )(live, parts)


def in_hbm(value):
    return pltpu.with_memory_space_constraint(value, pltpu.HBM)


def exchange(value, axes):
    return lax.all_to_all(value, axes, 0, 0)


def body(hidden, norm_gain, head_weight, targets, lengths):
    own_rows = hidden.shape[0]
    nx, nc = lax.axis_size("x"), lax.axis_size("c")
    plane = lax.axis_size(PLANE)
    block = plane * own_rows

    def turn(value, k):
        return lax.ppermute(value, "x", [(i, (i + k) % nx) for i in range(nx)])

    wide, narrow = norm(hidden, norm_gain, plane, WIDE)
    mine = exchange(wide, PLANE).reshape(block, WIDE)
    other_weight = lax.ppermute(head_weight, "c", [(0, 1), (1, 0)])
    column = jnp.concatenate([narrow, turn(narrow, 1), turn(narrow, nx - 1), turn(narrow, 2)], axis=0)
    mixed = exchange(jnp.broadcast_to(column[None], (plane, *column.shape)), PLANE).reshape(nx * block, -1)
    low, high = mine[:block // 2], mine[block // 2:]
    up_low, down_high = turn(low, 1), turn(high, nx - 1)
    up_high, down_low = turn(high, 1), turn(low, nx - 1)
    far_low, far_high = turn(up_low, 1), turn(down_high, nx - 1)
    ids = targets.reshape(nx * nc, block)
    shards = in_hbm(head_weight), in_hbm(other_weight)
    near, live = early_product(lengths, (low, high, up_low, up_high), *shards)
    late, early, wide_w = mixed_product(ids, near, mixed, *shards)
    stats = last_product(ids, late, early, (down_low, down_high, far_low, far_high), wide_w, lax.axis_size(("x", "z")))
    stats = join(exchange(stats, ("x", "z")), lax.axis_size(("c", "y")))
    stats = exchange(stats, ("c", "y"))
    token_loss, mean_loss = final_loss(live, stats, own_rows)
    return (token_loss, mean_loss.reshape(()))


def solution(mesh):
    split = Mesh(mesh.devices.reshape(4, 2, 8, 8), TOK_VOC)
    in_specs = (P(TOK_VOC, None), P(), P(TOK_VOC, None), P(), P())
    out_specs = (P(TOK_VOC), P())
    return jax.shard_map(body, mesh=split, in_specs=in_specs, out_specs=out_specs, check_vma=False)
```

```python
import jax
import jax.numpy as jnp
from jax import lax
from jax.experimental import pallas as pl
from jax.experimental.pallas import tpu as pltpu
from jax.sharding import Mesh
from jax.sharding import PartitionSpec as P

WINDOW = 32
TOK_VOC = ("x", "c", "z", "y")
PLANE = ("z", "y")
WIDE = 3840
STRIP = 64
SEGMENTS = ((0, 0), (0, 1), (1, 0), (2, 1), (2, 0), (1, 1), (3, 0), (3, 1))
VMEM_LIMIT = 12 * 2**20
WIDE_VMEM = 20 * 2**20


def params(limit=8 * 2**20):
    return pltpu.CompilerParams(vmem_limit_bytes=limit)


def whole(shape):
    return pl.BlockSpec(shape, lambda *_: (0,) * len(shape))


def scalars():
    return pl.BlockSpec(memory_space=pltpu.SMEM)


def dot_t(a, b):
    return lax.dot_general(a, b, (((1,), (1,)), ((), ())), preferred_element_type=jnp.float32)


def norm_kernel(hidden, gain, wide, narrow):
    values = hidden[...].astype(jnp.float32)
    meansq = jnp.mean(values * values, axis=1, keepdims=True)
    normed = (values * lax.rsqrt(meansq + 1e-06) * gain[...].reshape(1, -1)).astype(jnp.bfloat16)
    width = wide.shape[2]
    narrow[...] = normed[:, width:]
    for i in range(wide.shape[0]):
        wide[i] = normed[:, :width]


def norm(hidden, gain, copies, width):
    rows, depth = hidden.shape
    shapes = [(copies, rows, width), (rows, depth - width)]
    return pl.pallas_call(
        norm_kernel,
        in_specs=[whole(hidden.shape), whole(gain.shape)],
        out_specs=[whole(s) for s in shapes],
        out_shape=[jax.ShapeDtypeStruct(s, jnp.bfloat16) for s in shapes],
        compiler_params=params(),
        name="norm",
    )(in_hbm(hidden), in_hbm(gain))


def position(own_rows):
    x, c = lax.axis_index("x"), lax.axis_index("c")
    seat = lax.axis_index("z") * lax.axis_size("y") + lax.axis_index("y")
    return x, c, seat * own_rows


def sources(x):
    nx = lax.axis_size("x")
    return [lax.rem(x + nx - k, nx) for k in (0, 1, nx - 1, 2)]


def halves(one, two):
    lane = lax.broadcasted_iota(jnp.int32, one.shape, 1)
    return jnp.where(lane < 64, one, two)


def token_sums(targets, early, logits):
    vocab, tokens = logits.shape
    shard = vocab // 2
    x, c, seat = position(1)
    nc, plane = lax.axis_size("c"), lax.axis_size(PLANE)
    starts = [((x * nc + core) * plane + seat) * shard for core in (c, 1 - c)]
    own, up, down, far = [targets[pl.ds(source * nc + c, 1), :] for source in sources(x)]
    wanted = jnp.concatenate([own, halves(up, down)] if early else [halves(down, up), far], axis=1)
    expsum = jnp.zeros((8, tokens), jnp.float32)
    picked = jnp.zeros((8, tokens), jnp.float32)
    column = lax.broadcasted_iota(jnp.int32, (STRIP, tokens), 0)
    for r in range(0, vocab, STRIP):
        half, offset = divmod(r, shard)
        capped = 30.0 * jnp.tanh(logits[r:r + STRIP, :] / 30.0)
        hit = jnp.where(column == wanted - (starts[half] + offset), capped, 0.0)
        expsum += jnp.sum(jnp.exp(capped).reshape(STRIP // 8, 8, tokens), axis=0)
        picked += jnp.sum(hit.reshape(STRIP // 8, 8, tokens), axis=0)
    return jnp.sum(expsum, axis=0, keepdims=True), jnp.sum(picked, axis=0, keepdims=True)


def fetch(shards, kept, sems, spans):
    vocab = shards[0].shape[0]
    copies = []
    for i, (start, stop) in enumerate(spans):
        pair = []
        for j, shard in enumerate(shards):
            source = shard.at[:, start:stop]
            target = kept.at[j * vocab:(j + 1) * vocab, start:stop]
            pair.append(pltpu.make_async_copy(source, target, sems.at[2 * i + j]))
            pair[-1].start()
        copies.append(pair)
    return copies


def early_kernel(lengths, x0, x1, x2, x3, w0, w1, logits, live, weight, sems):
    wide = x0.shape[1]
    cut = wide // 256 * 128
    spans = ((0, cut), (cut, wide))
    copies = fetch((w0, w1), weight, sems, spans)
    lane = lax.broadcasted_iota(jnp.int32, (1, 128), 1)
    groups = live.shape[0] // 4
    count = 0
    for core in range(2):
        for k in range(groups):
            length = jnp.zeros((1, 128), jnp.int32)
            for j in range(128 // WINDOW):
                here = lengths[(k * 2 + core) * (128 // WINDOW) + j]
                count = count + here
                length = jnp.where(lane // WINDOW == j, here, length)
            i = core * groups + k
            live[i:i + 1, :] = jnp.where(lane % WINDOW < length, 1.0, 0.0)
    live[2 * groups:, :] = jnp.full((2 * groups, 128), count, jnp.int32).astype(jnp.float32)
    for i, span in enumerate(spans):
        for copy in copies[i]:
            copy.wait()
        cols = slice(*span)
        x = jnp.concatenate([x0[:, cols], x1[:, cols], x2[:, cols], x3[:, cols]], axis=0)
        part = dot_t(weight[:, cols], x)
        if i == 0:
            logits[...] = part
        else:
            logits[...] += part


INSIDE = pl.BlockSpec(memory_space=pltpu.VMEM)
OUTSIDE = pl.BlockSpec(memory_space=pltpu.HBM)


def early_product(lengths, xs, w0, w1):
    vocab = 2 * w0.shape[0]
    wide = xs[0].shape[1]
    tokens = sum(x.shape[0] for x in xs)
    return pl.pallas_call(
        early_kernel,
        in_specs=[scalars()] + [INSIDE] * 4 + [OUTSIDE] * 2,
        out_specs=[INSIDE] * 2,
        out_shape=[
            jax.ShapeDtypeStruct((vocab, tokens), jnp.float32),
            jax.ShapeDtypeStruct((16, 128), jnp.float32),
        ],
        scratch_shapes=[pltpu.VMEM((vocab, wide), w0.dtype), pltpu.SemaphoreType.DMA((4,))],
        compiler_params=params(WIDE_VMEM),
        cost_estimate=pl.CostEstimate(flops=2 * vocab * tokens * wide, bytes_accessed=10 * 2**20, transcendentals=0),
        name="early_product",
    )(lengths, *xs, w0, w1)


def mixed_kernel(targets, near, mixed, w0, w1, late, stat, kept, rows, logits, narrow_w, sems):
    tokens = mixed.shape[0]
    groups = tokens // 128
    early = logits.shape[1]
    half = tokens // 2
    vocab = w0.shape[0]
    wide = kept.shape[1]
    copies = [
        pltpu.make_async_copy(w.at[:, wide:], narrow_w.at[j * vocab:(j + 1) * vocab, :], sems.at[2 + j])
        for j, w in enumerate((w0, w1))
    ]
    for copy in copies:
        copy.start()
    others = fetch((w0, w1), kept, sems, ((0, wide),))
    row = lax.broadcasted_iota(jnp.int32, (half, half), 0)
    col = lax.broadcasted_iota(jnp.int32, (half, half), 1)
    inner = row & 63
    pick = (inner >> 1) * (2 * groups) + (row >> 6) * 2 + (inner & 1)
    chosen = jnp.where(col == pick, 1.0, 0.0).astype(jnp.bfloat16)
    for h in range(2):
        part = jnp.dot(chosen, mixed[h * half:(h + 1) * half, :], preferred_element_type=jnp.float32)
        for k in range(groups):
            place = SEGMENTS.index((k, h)) * 64
            rows[place:place + 64, :] = part[k * 64:(k + 1) * 64].astype(jnp.bfloat16)
    for copy in copies:
        copy.wait()
    late[...] = dot_t(narrow_w[...], rows[early:, :])
    logits[...] = near[...] + dot_t(narrow_w[...], rows[:early, :])
    for i, total in enumerate(token_sums(targets, True, logits)):
        for k in range(2):
            stat[2 * i + k:2 * i + k + 1, :] = total[:, k * 128:(k + 1) * 128]
    for copy in others[0]:
        copy.wait()


def mixed_product(targets, near, mixed, w0, w1):
    vocab, depth = 2 * w0.shape[0], w0.shape[1]
    tokens, narrow = mixed.shape
    early = near.shape[1]
    return pl.pallas_call(
        mixed_kernel,
        in_specs=[INSIDE] * 3 + [OUTSIDE] * 2,
        out_specs=[INSIDE] * 3,
        out_shape=[
            jax.ShapeDtypeStruct((vocab, tokens - early), jnp.float32),
            jax.ShapeDtypeStruct((8, 128), jnp.float32),
            jax.ShapeDtypeStruct((vocab, depth - narrow), w0.dtype),
        ],
        scratch_shapes=[
            pltpu.VMEM((tokens, narrow), jnp.bfloat16),
            pltpu.VMEM((vocab, early), jnp.float32),
            pltpu.VMEM((vocab, narrow), w0.dtype),
            pltpu.SemaphoreType.DMA((4,)),
        ],
        compiler_params=params(WIDE_VMEM),
        cost_estimate=pl.CostEstimate(flops=2 * vocab * tokens * narrow, bytes_accessed=12 * 2**20, transcendentals=0),
        name="mixed_product",
    )(targets, near, mixed, w0, w1)


def last_kernel(targets, late, early_stat, x0, x1, x2, x3, weight, out, logits, stat):
    logits[...] = late[...] + dot_t(weight[...], jnp.concatenate([x0[...], x1[...], x2[...], x3[...]], axis=0))
    origin = sources(lax.axis_index("x"))
    for i, total in enumerate(token_sums(targets, False, logits)):
        own, soon = early_stat[2 * i:2 * i + 1, :], early_stat[2 * i + 1:2 * i + 2, :]
        late_part, far = total[:, :128], total[:, 128:]
        for k, row in enumerate((own, halves(soon, late_part), halves(late_part, soon), far)):
            stat[pl.ds(origin[k] + 4 * i, 1), :] = row
    for i in range(out.shape[0]):
        out[i] = stat[...]


def last_product(targets, late, early_stat, xs, weight, copies):
    vocab, depth = weight.shape
    return pl.pallas_call(
        last_kernel,
        in_specs=[INSIDE] * 8,
        out_specs=INSIDE,
        out_shape=jax.ShapeDtypeStruct((copies, *early_stat.shape), jnp.float32),
        scratch_shapes=[pltpu.VMEM(late.shape, jnp.float32), pltpu.VMEM(early_stat.shape, jnp.float32)],
        compiler_params=params(VMEM_LIMIT),
        cost_estimate=pl.CostEstimate(flops=2 * vocab * 256 * depth, bytes_accessed=10 * 2**20, transcendentals=0),
        name="last_product",
    )(targets, late, early_stat, *xs, weight)


def join_kernel(parts, out):
    total = jnp.sum(parts[...], axis=0)
    for i in range(out.shape[0]):
        out[i] = total


def join(parts, copies):
    return pl.pallas_call(
        join_kernel,
        in_specs=[INSIDE],
        out_specs=INSIDE,
        out_shape=jax.ShapeDtypeStruct((copies, *parts.shape[1:]), jnp.float32),
        compiler_params=params(),
        name="join",
    )(parts)


def loss_kernel(live, parts, token_loss, mean_loss, loss):
    groups = parts.shape[1] // 2
    for core in range(2):
        total = jnp.sum(parts[core * parts.shape[0] // 2:(core + 1) * parts.shape[0] // 2], axis=0)
        rows = slice(core * groups, (core + 1) * groups)
        loss[rows, :] = live[rows, :] * (jnp.log(total[:groups]) - total[groups:])
    mean_loss[0] = jnp.sum(loss[...]) / live[2 * groups, 0]
    own_rows = token_loss.shape[0]
    x, c, seat = position(own_rows)
    own = loss[pl.ds(c * groups + x, 1), :]
    lane = lax.broadcasted_iota(jnp.int32, own.shape, 1)
    for i in range(own_rows):
        token_loss[i] = jnp.sum(jnp.where(lane == seat + i, own, 0.0))


def final_loss(live, parts, own_rows):
    return pl.pallas_call(
        loss_kernel,
        in_specs=[INSIDE] * 2,
        out_specs=[scalars(), scalars()],
        out_shape=[jax.ShapeDtypeStruct((own_rows,), jnp.float32), jax.ShapeDtypeStruct((1,), jnp.float32)],
        scratch_shapes=[pltpu.VMEM(parts.shape[1:], jnp.float32)],
        compiler_params=params(),
        name="final_loss",
    )(live, parts)


def in_hbm(value):
    return pltpu.with_memory_space_constraint(value, pltpu.HBM)


def exchange(value, axes):
    return lax.all_to_all(value, axes, 0, 0)


def body(hidden, norm_gain, head_weight, targets, lengths):
    own_rows = hidden.shape[0]
    nx, nc = lax.axis_size("x"), lax.axis_size("c")
    plane = lax.axis_size(PLANE)
    block = plane * own_rows

    def turn(value, k):
        return lax.ppermute(value, "x", [(i, (i + k) % nx) for i in range(nx)])

    wide, narrow = norm(hidden, norm_gain, plane, WIDE)
    mine = exchange(wide, PLANE).reshape(block, WIDE)
    other_weight = lax.ppermute(head_weight, "c", [(0, 1), (1, 0)])
    column = jnp.concatenate([narrow, turn(narrow, 1), turn(narrow, nx - 1), turn(narrow, 2)], axis=0)
    mixed = exchange(jnp.broadcast_to(column[None], (plane, *column.shape)), PLANE).reshape(nx * block, -1)
    low, high = mine[:block // 2], mine[block // 2:]
    up_low, down_high = turn(low, 1), turn(high, nx - 1)
    up_high, down_low = turn(high, 1), turn(low, nx - 1)
    far_low, far_high = turn(up_low, 1), turn(down_high, nx - 1)
    ids = targets.reshape(nx * nc, block)
    shards = in_hbm(head_weight), in_hbm(other_weight)
    near, live = early_product(lengths, (low, high, up_low, down_high), *shards)
    late, early, wide_w = mixed_product(ids, near, mixed, *shards)
    stats = last_product(ids, late, early, (down_low, up_high, far_low, far_high), wide_w, lax.axis_size(("x", "z")))
    stats = join(exchange(stats, ("x", "z")), lax.axis_size(("c", "y")))
    stats = exchange(stats, ("c", "y"))
    token_loss, mean_loss = final_loss(live, stats, own_rows)
    return (token_loss, mean_loss.reshape(()))


def solution(mesh):
    split = Mesh(mesh.devices.reshape(4, 2, 8, 8), TOK_VOC)
    in_specs = (P(TOK_VOC, None), P(), P(TOK_VOC, None), P(), P())
    out_specs = (P(TOK_VOC), P())
    return jax.shard_map(body, mesh=split, in_specs=in_specs, out_specs=out_specs, check_vma=False)
```
